128 devices in a mesh: dp: 1, node: 2 (over core), ep: 64 (over z, y, x).
Axes of the slice: x: 4, y: 4, z: 4, core: 2. Of those that a mesh axis runs over, the one named last changes fastest.
Arguments:
- tokens: bfloat16 [32768, 2048], P(('dp', 'node', 'ep'))
- expert_ids: int32 [32768, 8], P(('dp', 'node', 'ep'))
- route_w: float32 [32768, 8], P(('dp', 'node', 'ep'))
- node_slot: int32 [32768, 8], P(('dp', 'node', 'ep'))
- exp_slot: int32 [32768, 8], P(('dp', 'node', 'ep'))
- w_gate: bfloat16 [128, 2048, 768], P(('node', 'ep'))
- w_up: bfloat16 [128, 2048, 768], P(('node', 'ep'))
- w_down: bfloat16 [128, 768, 2048], P(('node', 'ep'))
Outputs:
- output: bfloat16 [32768, 2048], P(('dp', 'node', 'ep'))
All inputs are finite; a program needn't handle non-finite values.
Results may differ from the reference program's by a relative error of at most 0.00151.
Values are sent between devices in bfloat16 or wider.
A program may use at most 1 GiB of HBM per device.

```python
import jax
import jax.numpy as jnp
from jax import lax

D_MODEL = 2048
D_FF = 768
NUM_EXPERTS = 128
TOP_K = 8
TOK_DEV = 256
NODE_COUNT = 2
EP_SIZE = 64

NODE_LIMIT = max(1, min(TOP_K, NODE_COUNT // 2))
CAP_NODE = min(TOK_DEV, 8 * ((5 * TOK_DEV * NODE_LIMIT + 32 * NODE_COUNT - 1) // (32 * NODE_COUNT)))
CAP_EXP = 8 * ((5 * NODE_COUNT * TOK_DEV * TOP_K + 32 * NUM_EXPERTS - 1) // (32 * NUM_EXPERTS))
HOT_ROWS = min(CAP_NODE, (CAP_EXP + NODE_COUNT - 1) // NODE_COUNT)
EXP_NODE = NUM_EXPERTS // NODE_COUNT
NUM_DEV = NODE_COUNT * EP_SIZE
TOK_ALL = NUM_DEV * TOK_DEV


def rank_within(flag_rows, priority):
    sort_order = jnp.argsort(-priority, axis=1)
    flags_sorted = jnp.take_along_axis(flag_rows, sort_order[:, :, None], axis=1)
    rank_sorted = jnp.cumsum(flags_sorted, axis=1) - flags_sorted
    back_order = jnp.argsort(sort_order, axis=1)
    return jnp.take_along_axis(rank_sorted, back_order[:, :, None], axis=1)


def route_draw(key_route):
    key_node, key_exp, key_npri, key_epri = jax.random.split(key_route, 4)
    row_ids = jnp.arange(TOK_ALL)
    local_row = row_ids % TOK_DEV
    src_ep = (row_ids // TOK_DEV) % EP_SIZE
    src_node = row_ids // (TOK_DEV * EP_SIZE)
    hot_row = (src_ep == 0) & ((src_node == 0) | (local_row < HOT_ROWS))
    node_ids = jnp.arange(NODE_COUNT)
    node_score = jax.random.randint(key_node, (TOK_ALL, NODE_COUNT), 0, 1024)
    node_score = node_score + jnp.where(node_ids == 0, 192, 0)[None, :]
    node_score = node_score + jnp.where(hot_row[:, None] & (node_ids == 0)[None, :], 4096, 0)
    node_score = node_score * NODE_COUNT + node_ids[None, :]
    top_vals = lax.top_k(node_score, NODE_LIMIT)[0]
    node_open = node_score >= top_vals[:, NODE_LIMIT - 1:NODE_LIMIT]
    exp_ids = jnp.arange(NUM_EXPERTS)
    exp_score = jax.random.randint(key_exp, (TOK_ALL, NUM_EXPERTS), 0, 1024)
    exp_score = exp_score + (((exp_ids * 5) % 8) * 48)[None, :]
    exp_score = exp_score + jnp.where(hot_row[:, None] & (exp_ids == 0)[None, :], 8192, 0)
    exp_open = jnp.repeat(node_open, EXP_NODE, axis=1)
    exp_score = jnp.where(exp_open, exp_score, -1) * NUM_EXPERTS + exp_ids[None, :]
    expert_ids = lax.top_k(exp_score, TOP_K)[1]
    node_of = expert_ids // EXP_NODE
    node_used = jnp.zeros((TOK_ALL, NODE_COUNT), jnp.int32).at[row_ids[:, None], node_of].set(1)
    node_pri = hot_row.astype(jnp.int32) * TOK_ALL + jax.random.permutation(key_npri, TOK_ALL)
    node_rank = rank_within(node_used.reshape(NUM_DEV, TOK_DEV, NODE_COUNT), node_pri.reshape(NUM_DEV, TOK_DEV)).reshape(TOK_ALL, NODE_COUNT)
    node_pos = jnp.take_along_axis(node_rank, node_of, axis=1)
    node_kept = node_pos < CAP_NODE
    node_slot = jnp.where(node_kept, node_pos, -1)
    exp_hot = jnp.zeros((TOK_ALL, NUM_EXPERTS), jnp.int32).at[row_ids[:, None], expert_ids].set(node_kept.astype(jnp.int32))
    group_rows = row_ids.reshape(NODE_COUNT, EP_SIZE, TOK_DEV).transpose(1, 0, 2).reshape(EP_SIZE, NODE_COUNT * TOK_DEV)
    exp_pri = jax.random.permutation(key_epri, TOK_ALL)
    exp_rank_group = rank_within(exp_hot[group_rows], exp_pri[group_rows])
    exp_rank = jnp.zeros((TOK_ALL, NUM_EXPERTS), jnp.int32).at[group_rows.reshape(-1)].set(exp_rank_group.reshape(TOK_ALL, NUM_EXPERTS).astype(jnp.int32))
    exp_pos = jnp.take_along_axis(exp_rank, expert_ids, axis=1)
    exp_slot = jnp.where(node_kept & (exp_pos < CAP_EXP), exp_pos, -1)
    return expert_ids.astype(jnp.int32), node_slot.astype(jnp.int32), exp_slot.astype(jnp.int32)


def setup_inputs(seed: int = 0, part: int = 0) -> dict:
    key_all = jax.random.key(seed)
    key_part = jax.random.fold_in(key_all, part)
    key_route, key_tok, key_gate = jax.random.split(key_part, 3)
    key_wg, key_wu, key_wd = jax.random.split(jax.random.fold_in(key_all, 1000003), 3)
    expert_ids, node_slot, exp_slot = route_draw(key_route)
    tokens = jax.random.normal(key_tok, (TOK_ALL, D_MODEL), jnp.float32).astype(jnp.bfloat16)
    gate_raw = jax.random.uniform(key_gate, (TOK_ALL, TOP_K), jnp.float32, 0.5, 1.5)
    route_w = gate_raw * TOP_K ** -0.5
    w_gate = (jax.random.normal(key_wg, (NUM_EXPERTS, D_MODEL, D_FF), jnp.float32) * D_MODEL ** -0.5).astype(jnp.bfloat16)
    w_up = (jax.random.normal(key_wu, (NUM_EXPERTS, D_MODEL, D_FF), jnp.float32) * D_MODEL ** -0.5).astype(jnp.bfloat16)
    w_down = (jax.random.normal(key_wd, (NUM_EXPERTS, D_FF, D_MODEL), jnp.float32) * D_FF ** -0.5).astype(jnp.bfloat16)
    return {'tokens': tokens, 'expert_ids': expert_ids, 'route_w': route_w, 'node_slot': node_slot, 'exp_slot': exp_slot, 'w_gate': w_gate, 'w_up': w_up, 'w_down': w_down}


def reference(tokens, expert_ids, route_w, node_slot, exp_slot, w_gate, w_up, w_down):
    row_ids = jnp.arange(TOK_ALL)
    src_ep = (row_ids // TOK_DEV) % EP_SIZE
    kept_choice = (node_slot >= 0) & (exp_slot >= 0)
    buf_size = NUM_EXPERTS * EP_SIZE * CAP_EXP
    buf_pos = (expert_ids * EP_SIZE + src_ep[:, None]) * CAP_EXP + exp_slot
    buf_pos = jnp.where(kept_choice, buf_pos, buf_size)
    src_row = jnp.full((buf_size,), TOK_ALL - 1, jnp.int32).at[buf_pos.reshape(-1)].set(jnp.repeat(row_ids, TOP_K).astype(jnp.int32), mode='drop')
    src_row = src_row.reshape(NUM_EXPERTS, EP_SIZE * CAP_EXP)

    def expert_ffn(operands):
        row_sel, gate_mat, up_mat, down_mat = operands
        rows_in = tokens[row_sel]
        gate_act = jnp.dot(rows_in, gate_mat, preferred_element_type=jnp.float32)
        up_act = jnp.dot(rows_in, up_mat, preferred_element_type=jnp.float32)
        hidden = (jax.nn.silu(gate_act) * up_act).astype(jnp.bfloat16)
        return jnp.dot(hidden, down_mat, preferred_element_type=jnp.float32).astype(jnp.bfloat16)

    exp_out = lax.map(expert_ffn, (src_row, w_gate, w_up, w_down)).reshape(buf_size, D_MODEL)
    safe_pos = jnp.minimum(buf_pos, buf_size - 1)
    weight = jnp.where(kept_choice, route_w, 0.0)
    node_of = expert_ids // EXP_NODE
    same_node = node_of[:, :, None] == node_of[:, None, :]
    earlier = jnp.arange(TOP_K)[None, :] < jnp.arange(TOP_K)[:, None]
    first_on = jnp.logical_not(jnp.any(same_node & earlier[None], axis=2)) & (node_slot >= 0)
    node_on = first_on.astype(jnp.float32)
    mix_wt = jnp.where(same_node, weight[:, None, :], 0.0)

    def combine_block(operands):
        pos_blk, mix_blk, on_blk = operands
        picked = exp_out[pos_blk].astype(jnp.float32)
        partial = jnp.einsum('tjl,tld->tjd', mix_blk, picked).astype(jnp.bfloat16)
        return jnp.einsum('tj,tjd->td', on_blk, partial.astype(jnp.float32)).astype(jnp.bfloat16)

    out_rows = lax.map(combine_block, (safe_pos.reshape(NUM_DEV, TOK_DEV, TOP_K), mix_wt.reshape(NUM_DEV, TOK_DEV, TOP_K, TOP_K), node_on.reshape(NUM_DEV, TOK_DEV, TOP_K)))
    return out_rows.reshape(TOK_ALL, D_MODEL)
```

```python
import functools

import jax
import jax.numpy as jnp
from jax import lax
from jax.experimental import pallas as pl
from jax.experimental.pallas import tpu as pltpu
from jax.sharding import PartitionSpec as P

MESH = pl.DeviceIdType.MESH
SIDE = 4
SHIFTS = (1, 3, 2)
ROUTES = ((2, 1, 0), (1, 0, 2), (0, 2, 1))
BLK = 8


def part_columns(d_model):
    tiles = d_model // 128
    base, extra = tiles // 3, tiles % 3
    cols, at = [], 0
    for k in range(3):
        width = (base + (1 if k >= 3 - extra else 0)) * 128
        cols.append((at, width))
        at += width
    return cols


def moe_kernel(dims, tok_hbm, meta_hbm, metat_hbm, wg_hbm, wu_hbm, wd_hbm, out_ref, mid_d, mid_r,
               tok, meta, metat, wg, wu, wd, send0, hop, work, back, hid, acc, p_send, p_recv,
               in_sem, w_sem, own_sem, send_sem, recv_sem, pair_send, pair_recv):
    n_chunks, n_ep, node_stride, slot_stride, top_k = dims
    tok_dev, d_model = tok_hbm.shape
    d_ff = wg_hbm.shape[1]
    rows = n_ep * BLK
    node = lax.axis_index("node")
    ep = lax.axis_index("ep")
    pos = (ep // (SIDE * SIDE), (ep // SIDE) % SIDE, ep % SIDE)
    cols = part_columns(d_model)
    other = 1 - node

    def peer(dim, shift):
        at = [pos[0], pos[1], pos[2]]
        at[dim] = (pos[dim] + shift) % SIDE
        return (at[0] * SIDE + at[1]) * SIDE + at[2]

    def plane(ref, chunk, dim, index, part):
        c0, width = cols[part]
        idx = [chunk, slice(None), slice(None), slice(None), slice(None), pl.ds(c0, width)]
        idx[1 + dim] = index
        return ref.at[tuple(idx)]

    weights = [pltpu.make_async_copy(s, d, w_sem.at[i]) for i, (s, d) in enumerate(((wg_hbm, wg), (wu_hbm, wu), (wd_hbm, wd)))]
    inputs = ((tok_hbm, tok), (meta_hbm, meta), (metat_hbm, metat))
    local_in = [pltpu.make_async_copy(s, d.at[node], in_sem.at[i]) for i, (s, d) in enumerate(inputs)]
    pair_in = [pltpu.make_async_remote_copy(src_ref=s, dst_ref=d.at[node], send_sem=pair_send.at[i], recv_sem=pair_recv.at[i],
                                            device_id={"node": other}, device_id_type=MESH) for i, (s, d) in enumerate(inputs)]
    for c in local_in:
        c.start()
    barrier = pltpu.get_barrier_semaphore()
    pl.semaphore_signal(barrier, inc=1, device_id={"node": other}, device_id_type=MESH)
    for dim in range(3):
        for shift in SHIFTS:
            pl.semaphore_signal(barrier, inc=1, device_id={"ep": peer(dim, shift)}, device_id_type=MESH)
    pl.semaphore_wait(barrier, 1 + 3 * len(SHIFTS))
    for c in pair_in:
        c.start()
    for c in weights:
        c.start()
    acc[...] = jnp.zeros_like(acc)
    for c in local_in:
        c.wait()
    for c in pair_in:
        c.wait()

    stages = ((send0, 2, hop, 0), (hop, n_chunks, mid_d, 1), (mid_d, n_chunks, work, 2),
              (work, n_chunks, hop, 2), (hop, n_chunks, mid_r, 1), (mid_r, n_chunks, back, 0))

    def copies(stage, chunk):
        src, src_slots, dst, leg = stages[stage]
        src_chunk = chunk % src_slots if src_slots == 2 else chunk
        remote, local = [], []
        for part in range(3):
            dim = ROUTES[part][leg]
            for v, shift in enumerate(SHIFTS):
                remote.append(pltpu.make_async_remote_copy(
                    src_ref=plane(src, src_chunk, dim, (pos[dim] + shift) % SIDE, part),
                    dst_ref=plane(dst, chunk, dim, pos[dim], part),
                    send_sem=send_sem.at[stage, chunk % 2, part, v],
                    recv_sem=recv_sem.at[stage, chunk, part, v],
                    device_id={"ep": peer(dim, shift)}, device_id_type=MESH))
            local.append(pltpu.make_async_copy(
                plane(src, src_chunk, dim, pos[dim], part), plane(dst, chunk, dim, pos[dim], part),
                own_sem.at[stage, chunk % 2, part]))
        return remote, local

    def launch(stage, chunk):
        remote, local = copies(stage, chunk)
        for c in remote:
            c.start()
        for c in local:
            c.start()

    def finish(stage, chunk):
        remote, local = copies(stage, chunk)
        for c in remote:
            c.wait()
        for c in local:
            c.wait()

    base = (node * node_stride).astype(jnp.float32)

    def gather(chunk):
        row = lax.broadcasted_iota(jnp.int32, (rows, tok_dev), 0)
        want = ((row // BLK) * slot_stride + row % BLK + chunk * BLK).astype(jnp.float32) + base
        picks = []
        for n in range(2):
            hit = jnp.zeros((rows, tok_dev), jnp.float32)
            for j in range(top_k):
                hit = jnp.where(metat[n, j:j + 1, :] == want, 1.0, hit)
            picks.append(hit.astype(jnp.bfloat16))
        width = 512
        for n in range(d_model // width):
            block = (jnp.dot(picks[0], tok[0, :, n * width:(n + 1) * width], preferred_element_type=jnp.float32)
                     + jnp.dot(picks[1], tok[1, :, n * width:(n + 1) * width], preferred_element_type=jnp.float32))
            send0[chunk % 2, :, :, :, :, n * width:(n + 1) * width] = block.reshape(SIDE, SIDE, SIDE, BLK, width).astype(jnp.bfloat16)

    def ffn(chunk):
        width = 256

        def up(n, carry):
            at = pl.ds(pl.multiple_of(n * width, width), width)
            x = work[chunk].reshape(rows, d_model)
            g = jnp.dot(x, wg[:, at], preferred_element_type=jnp.float32)
            u = jnp.dot(x, wu[:, at], preferred_element_type=jnp.float32)
            hid[:, at] = (jax.nn.silu(g) * u).astype(jnp.bfloat16)
            return carry

        lax.fori_loop(0, d_ff // width, up, 0)

        def down(n, carry):
            at = pl.ds(pl.multiple_of(n * width, width), width)
            y = jnp.dot(hid[...], wd[:, at], preferred_element_type=jnp.float32)
            work[chunk, :, :, :, :, at] = y.reshape(SIDE, SIDE, SIDE, BLK, width).astype(jnp.bfloat16)
            return carry

        lax.fori_loop(0, d_model // width, down, 0)

    def combine(chunk):
        lane = lax.broadcasted_iota(jnp.int32, (tok_dev, rows), 1)
        want = ((lane // BLK) * slot_stride + lane % BLK + chunk * BLK).astype(jnp.float32) + base
        width = 512
        for n in range(2):
            mix = jnp.zeros((tok_dev, rows), jnp.float32)
            for j in range(top_k):
                mix = jnp.where(meta[n, :, j:j + 1] == want, meta[n, :, top_k + j:top_k + j + 1], mix)
            hi = mix.astype(jnp.bfloat16)
            rest = mix - hi.astype(jnp.float32)
            mid = rest.astype(jnp.bfloat16)
            lo = (rest - mid.astype(jnp.float32)).astype(jnp.bfloat16)
            for q in range(d_model // width):
                at = slice(q * width, (q + 1) * width)
                y = back[chunk, :, :, :, :, at].reshape(rows, width)
                add = jnp.dot(lo, y, preferred_element_type=jnp.float32)
                add = add + jnp.dot(mid, y, preferred_element_type=jnp.float32)
                add = add + jnp.dot(hi, y, preferred_element_type=jnp.float32)
                acc[n, :, at] += add

    def step(t, carry):
        @pl.when(t < n_chunks)
        def _():
            gather(t)
            launch(0, t)

        for stage in range(1, 7):
            chunk = t - stage

            @pl.when((chunk >= 0) & (chunk < n_chunks))
            def _():
                finish(stage - 1, chunk)
                if stage == 3:
                    @pl.when(chunk == 0)
                    def _():
                        for c in weights:
                            c.wait()
                    ffn(chunk)
                if stage < 6:
                    launch(stage, chunk)
                else:
                    combine(chunk)
        return carry

    lax.fori_loop(0, n_chunks + 6, step, 0)

    p_send[...] = acc[other].astype(jnp.bfloat16)
    share = pltpu.make_async_remote_copy(src_ref=p_send, dst_ref=p_recv, send_sem=pair_send.at[3], recv_sem=pair_recv.at[3],
                                         device_id={"node": other}, device_id_type=MESH)
    share.start()
    mine = acc[node].astype(jnp.bfloat16).astype(jnp.float32)
    share.wait()
    out_ref[...] = (mine + p_recv[...].astype(jnp.float32)).astype(jnp.bfloat16)


def solution(mesh):
    n_nodes = mesh.shape['node']
    n_ep = mesh.shape['ep']
    row_spec = P(('dp', 'node', 'ep'), None)
    exp_spec = P(('node', 'ep'), None, None)

    def local_layer(tokens, expert_ids, route_w, node_slot, exp_slot, w_gate, w_up, w_down):
        tok_dev, d_model = tokens.shape
        top_k = expert_ids.shape[1]
        d_ff = w_gate.shape[2]
        n_exp = w_gate.shape[0] * n_ep * n_nodes
        cap_exp = 8 * ((5 * n_nodes * tok_dev * top_k + 32 * n_exp - 1) // (32 * n_exp))
        n_chunks = cap_exp // BLK
        slot_stride = 64
        node_stride = n_ep * slot_stride
        rows = n_ep * BLK

        kept = (node_slot >= 0) & (exp_slot >= 0)
        code = jnp.where(kept, expert_ids * slot_stride + exp_slot, -1).astype(jnp.float32)
        weight = jnp.where(kept, route_w, 0.0)
        meta = jnp.pad(jnp.concatenate([code, weight], axis=1), ((0, 0), (0, 128 - 2 * top_k)))
        metat = code.T

        cube = (SIDE, SIDE, SIDE, BLK, d_model)
        bf16, f32 = jnp.bfloat16, jnp.float32
        any_spec = pl.BlockSpec(memory_space=pl.ANY)
        out, _, _ = pl.pallas_call(
            functools.partial(moe_kernel, (n_chunks, n_ep, node_stride, slot_stride, top_k)),
            name="moe_layer",
            out_shape=(jax.ShapeDtypeStruct((tok_dev, d_model), bf16),
                       jax.ShapeDtypeStruct((n_chunks,) + cube, bf16),
                       jax.ShapeDtypeStruct((n_chunks,) + cube, bf16)),
            in_specs=[any_spec] * 6,
            out_specs=(pl.BlockSpec(memory_space=pltpu.VMEM), any_spec, any_spec),
            scratch_shapes=[
                pltpu.VMEM((2, tok_dev, d_model), bf16),
                pltpu.VMEM((2, tok_dev, 128), f32),
                pltpu.VMEM((2, top_k, tok_dev), f32),
                pltpu.VMEM((d_model, d_ff), bf16),
                pltpu.VMEM((d_model, d_ff), bf16),
                pltpu.VMEM((d_ff, d_model), bf16),
                pltpu.VMEM((2,) + cube, bf16),
                pltpu.VMEM((n_chunks,) + cube, bf16),
                pltpu.VMEM((n_chunks,) + cube, bf16),
                pltpu.VMEM((n_chunks,) + cube, bf16),
                pltpu.VMEM((rows, d_ff), bf16),
                pltpu.VMEM((2, tok_dev, d_model), f32),
                pltpu.VMEM((tok_dev, d_model), bf16),
                pltpu.VMEM((tok_dev, d_model), bf16),
                pltpu.SemaphoreType.DMA((3,)),
                pltpu.SemaphoreType.DMA((3,)),
                pltpu.SemaphoreType.DMA((6, 2, 3)),
                pltpu.SemaphoreType.DMA((6, 2, 3, 3)),
                pltpu.SemaphoreType.DMA((6, n_chunks, 3, 3)),
                pltpu.SemaphoreType.DMA((4,)),
                pltpu.SemaphoreType.DMA((4,)),
            ],
            compiler_params=pltpu.CompilerParams(collective_id=0, has_side_effects=True, vmem_limit_bytes=63 * 2**20),
        )(tokens, meta, metat, w_gate[0], w_up[0], w_down[0])
        return out

    return jax.shard_map(local_layer, mesh=mesh, in_specs=(row_spec,) * 5 + (exp_spec,) * 3, out_specs=row_spec, check_vma=False)
```

```python
import functools

import jax
import jax.numpy as jnp
from jax import lax
from jax.experimental import pallas as pl
from jax.experimental.pallas import tpu as pltpu
from jax.sharding import PartitionSpec as P

MESH = pl.DeviceIdType.MESH
SIDE = 4
SHIFTS = (1, 3, 2)
ROUTES = ((2, 1, 0), (1, 0, 2), (0, 2, 1))
STRIDE = (16, 4, 1)
BLK = 8
SLOTS = 64
NT = (((1,), (1,)), ((), ()))
TN = (((0,), (0,)), ((), ()))


def part_columns(d_model):
    tiles = d_model // 128
    base, extra = tiles // 3, tiles % 3
    cols, at = [], 0
    for k in range(3):
        width = (base + (1 if k >= 3 - extra else 0)) * 128
        cols.append((at, width))
        at += width
    return cols


def moe_kernel(n_chunks, ids_hbm, rw_hbm, ns_hbm, es_hbm, tok_hbm, wg_hbm, wu_hbm, wd_hbm, out_ref, mid_d, mid_r,
               ids, rw, ns, es, tok, pick, rg0, rg1, rg2, own_codes, codes, c_send, feat, f_send, r_send, p_recv,
               wg, wu, wd, send1, hop, work, back, hid, acc,
               in_sem, w_sem, own_sem, send_sem, recv_sem, pair_send, pair_recv, a_send, a_recv, b_send, b_recv, c_ssem, c_rsem):
    f32, bf16 = jnp.float32, jnp.bfloat16
    tok_dev, d_model = tok_hbm.shape
    d_ff = wg_hbm.shape[1]
    top_k = ids_hbm.shape[0]
    n_ep = SIDE ** 3
    rows = n_ep * BLK
    cap = feat.shape[1]
    half = cap // 2
    node = lax.axis_index("node")
    other = 1 - node
    ep = lax.axis_index("ep")
    pos = (ep // (SIDE * SIDE), (ep // SIDE) % SIDE, ep % SIDE)
    cols = part_columns(d_model)
    rings = (rg0, rg1, rg2)

    def peer(dim, shift):
        at = [pos[0], pos[1], pos[2]]
        at[dim] = (pos[dim] + shift) % SIDE
        return (at[0] * SIDE + at[1]) * SIDE + at[2]

    def to_ep(src, dst, ssem, rsem, dim, shift):
        return pltpu.make_async_remote_copy(src_ref=src, dst_ref=dst, send_sem=ssem, recv_sem=rsem,
                                            device_id={"ep": peer(dim, shift)}, device_id_type=MESH)

    def to_pair(src, dst, i):
        return pltpu.make_async_remote_copy(src_ref=src, dst_ref=dst, send_sem=pair_send.at[i], recv_sem=pair_recv.at[i],
                                            device_id={"node": other}, device_id_type=MESH)

    inputs = [pltpu.make_async_copy(s, d, in_sem.at[i]) for i, (s, d) in enumerate(
        ((ids_hbm, ids), (rw_hbm, rw), (ns_hbm, ns), (es_hbm, es), (tok_hbm, tok)))]
    weights = [pltpu.make_async_copy(s, d, w_sem.at[i]) for i, (s, d) in enumerate(((wg_hbm, wg), (wu_hbm, wu), (wd_hbm, wd)))]
    for c in inputs:
        c.start()
    barrier = pltpu.get_barrier_semaphore()
    pl.semaphore_signal(barrier, inc=1, device_id={"node": other}, device_id_type=MESH)
    for dim in range(3):
        for shift in SHIFTS:
            pl.semaphore_signal(barrier, inc=1, device_id={"ep": peer(dim, shift)}, device_id_type=MESH)
    for c in inputs:
        c.wait()

    def route(m):
        on = (ids[...] >= m * n_ep) & (ids[...] < (m + 1) * n_ep)
        slot = jnp.max(jnp.where(on, ns[...], -1), axis=0, keepdims=True)
        kept = on & (ns[...] >= 0) & (es[...] >= 0)
        a = jnp.where(kept, (ids[...] - m * n_ep) * SLOTS, 0).astype(f32)
        b = jnp.where(kept, es[...] + 1, 0).astype(f32)
        w = jnp.where(kept, rw[...], 0.0)
        w1 = w.astype(bf16).astype(f32)
        w2 = (w - w1).astype(bf16).astype(f32)
        w3 = w - w1 - w2
        fill = jnp.zeros((128 - 2 * top_k, tok_dev), f32)
        parts = [jnp.concatenate([p, q, fill], axis=0).astype(bf16) for p, q in ((a, w1), (b, w2), (jnp.zeros_like(a), w3))]
        hot = jnp.where(lax.broadcasted_iota(jnp.int32, (tok_dev, tok_dev), 0) == slot, 1.0, 0.0).astype(bf16)
        pick[m] = hot[:cap]
        code = sum(lax.dot_general(p, hot, NT, preferred_element_type=f32) for p in parts[:2])[:top_k]
        by_row = sum(lax.dot_general(hot[:cap], p, NT, preferred_element_type=f32) for p in parts[::-1])
        return code, by_row

    own_code, own_feat = route(node)
    for part in range(3):
        c0, width = cols[part]
        rings[part][pos[ROUTES[part][0]], node] = jnp.dot(
            pick[node], tok[:, c0:c0 + width], preferred_element_type=f32).astype(bf16)
    pl.semaphore_wait(barrier, 1 + 3 * len(SHIFTS))

    def ring_copies(part, n):
        dim, ring = ROUTES[part][0], rings[part]
        i = pos[dim]
        first = [to_ep(ring.at[i, n], ring.at[i, n], a_send.at[part, n, v], a_recv.at[part, n, v], dim, (1, 3)[v]) for v in range(2)]
        onward = []
        for v in range(2):
            k = (i + (3, 1)[v]) % SIDE
            span = pl.ds(v * half, half)
            onward.append(to_ep(ring.at[k, n, span], ring.at[k, n, span], b_send.at[part, n, v], b_recv.at[part, n, v], dim, (1, 3)[v]))
        return first, onward

    for part in range(3):
        for c in ring_copies(part, node)[0]:
            c.start()
    own_codes[node] = own_code
    feat[node] = own_feat
    far_code, far_feat = route(other)
    r_send[...] = jnp.dot(pick[other], tok[...], preferred_element_type=f32).astype(bf16)
    c_send[...] = far_code
    f_send[...] = far_feat
    pair = [to_pair(r_send.at[:, pl.ds(*cols[part])], rings[part].at[pos[ROUTES[part][0]], node], part) for part in range(3)]
    pair.append(to_pair(c_send, own_codes.at[node], 3))
    pair.append(to_pair(f_send, feat.at[node], 4))
    for c in pair:
        c.start()
    for c in weights:
        c.start()
    acc[...] = jnp.zeros_like(acc)
    for c in pair:
        c.wait()
    for part in range(3):
        for c in ring_copies(part, other)[0]:
            c.start()
    code_copies = [to_ep(own_codes, codes.at[dim, pos[dim]], c_ssem.at[dim, v], c_rsem.at[dim, v], dim, shift)
                   for dim in range(3) for v, shift in enumerate(SHIFTS)]
    for c in code_copies:
        c.start()
    for dim in range(3):
        codes[dim, pos[dim]] = own_codes[...]
    for n in (node, other):
        for part in range(3):
            first, onward = ring_copies(part, n)
            for v in range(2):
                first[v].wait()
                onward[v].start()
    for c in code_copies:
        c.wait()

    stages = ((send1, mid_d, 1), (mid_d, work, 2), (work, hop, 2), (hop, mid_r, 1), (mid_r, back, 0))

    def plane(ref, chunk, dim, index, part):
        c0, width = cols[part]
        idx = [chunk, slice(None), slice(None), slice(None), slice(None), pl.ds(c0, width)]
        idx[1 + dim] = index
        return ref.at[tuple(idx)]

    def copies(stage, chunk):
        src, dst, leg = stages[stage]
        src_chunk = chunk % 2 if stage == 0 else chunk
        remote, local = [], []
        for part in range(3):
            dim = ROUTES[part][leg]
            for v, shift in enumerate(SHIFTS):
                remote.append(to_ep(plane(src, src_chunk, dim, (pos[dim] + shift) % SIDE, part),
                                    plane(dst, chunk, dim, pos[dim], part),
                                    send_sem.at[stage, chunk % 2, part, v], recv_sem.at[stage, chunk, part, v], dim, shift))
            local.append(pltpu.make_async_copy(
                plane(src, src_chunk, dim, pos[dim], part), plane(dst, chunk, dim, pos[dim], part),
                own_sem.at[stage, chunk % 2, part]))
        return remote, local

    def launch(stage, chunk):
        remote, local = copies(stage, chunk)
        for c in remote:
            c.start()
        for c in local:
            c.start()

    def finish(stage, chunk):
        remote, local = copies(stage, chunk)
        for c in remote:
            c.wait()
        for c in local:
            c.wait()

    def gather(chunk):
        for v in (0, 3, 1, 2):
            if v == 2:
                @pl.when(chunk == 0)
                def _():
                    for n in (node, other):
                        for part in range(3):
                            for c in ring_copies(part, n)[1]:
                                c.wait()
            for part in range(3):
                dim = ROUTES[part][0]
                k = (pos[dim] + v) % SIDE
                c0, width = cols[part]
                o0, o1 = [d for d in range(3) if d != dim]
                r = lax.broadcasted_iota(jnp.int32, (SIDE * SIDE * BLK, cap), 0)
                expert = pos[dim] * STRIDE[dim] + (r >> 5) * STRIDE[o0] + ((r >> 3) & 3) * STRIDE[o1]
                want = (expert * SLOTS + (r & 7) + chunk * BLK + 1).astype(f32)
                block = None
                for n in range(2):
                    hit = jnp.zeros(want.shape, f32)
                    for j in range(top_k):
                        hit = jnp.where(codes[dim, k, n, j:j + 1, :cap] == want, 1.0, hit)
                    got = jnp.dot(hit.astype(bf16), rings[part][k, n], preferred_element_type=f32)
                    block = got if block is None else block + got
                idx = [chunk % 2, slice(None), slice(None), slice(None), slice(None), slice(c0, c0 + width)]
                idx[1 + dim] = k
                send1[tuple(idx)] = block.reshape(SIDE, SIDE, BLK, width).astype(bf16)

    def ffn(chunk):
        width = 256

        def up(n, carry):
            at = pl.ds(pl.multiple_of(n * width, width), width)
            x = work[chunk].reshape(rows, d_model)
            g = jnp.dot(x, wg[:, at], preferred_element_type=f32)
            u = jnp.dot(x, wu[:, at], preferred_element_type=f32)
            hid[:, at] = (jax.nn.silu(g) * u).astype(bf16)
            return carry

        lax.fori_loop(0, d_ff // width, up, 0)

        def down(n, carry):
            at = pl.ds(pl.multiple_of(n * width, width), width)
            y = jnp.dot(hid[...], wd[:, at], preferred_element_type=f32)
            work[chunk, :, :, :, :, at] = y.reshape(SIDE, SIDE, SIDE, BLK, width).astype(bf16)
            return carry

        lax.fori_loop(0, d_model // width, down, 0)

    def combine(chunk):
        lane = lax.broadcasted_iota(jnp.int32, (cap, rows), 1)
        want = ((lane >> 3) * SLOTS + (lane & 7) + chunk * BLK + 1).astype(f32)
        width = 512
        for n in range(2):
            mix = jnp.zeros((cap, rows), f32)
            for j in range(top_k):
                mix = jnp.where(feat[n, :, j:j + 1] == want, feat[n, :, top_k + j:top_k + j + 1], mix)
            hi = mix.astype(bf16)
            rest = mix - hi.astype(f32)
            mid = rest.astype(bf16)
            lo = (rest - mid.astype(f32)).astype(bf16)
            for q in range(d_model // width):
                at = slice(q * width, (q + 1) * width)
                y = back[chunk, :, :, :, :, at].reshape(rows, width)
                add = jnp.dot(lo, y, preferred_element_type=f32)
                add = add + jnp.dot(mid, y, preferred_element_type=f32)
                add = add + jnp.dot(hi, y, preferred_element_type=f32)
                acc[n, :, at] += add

    def step(t, carry):
        @pl.when(t < n_chunks)
        def _():
            gather(t)
            launch(0, t)

        for stage in range(1, 6):
            chunk = t - stage

            @pl.when((chunk >= 0) & (chunk < n_chunks))
            def _():
                finish(stage - 1, chunk)
                if stage == 2:
                    @pl.when(chunk == 0)
                    def _():
                        for c in weights:
                            c.wait()
                    ffn(chunk)
                if stage < 5:
                    launch(stage, chunk)
                else:
                    combine(chunk)
        return carry

    lax.fori_loop(0, n_chunks + 5, step, 0)

    r_send[...] = acc[other].astype(bf16)
    share = to_pair(r_send, p_recv, 5)
    share.start()
    mine = lax.dot_general(pick[node], acc[node].astype(bf16), TN, preferred_element_type=f32)
    share.wait()
    theirs = lax.dot_general(pick[other], p_recv[...], TN, preferred_element_type=f32)
    out_ref[...] = (mine + theirs).astype(bf16)


def solution(mesh):
    n_nodes = mesh.shape['node']
    n_ep = mesh.shape['ep']
    row_spec = P(('dp', 'node', 'ep'), None)
    exp_spec = P(('node', 'ep'), None, None)

    def local_layer(tokens, expert_ids, route_w, node_slot, exp_slot, w_gate, w_up, w_down):
        tok_dev, d_model = tokens.shape
        top_k = expert_ids.shape[1]
        d_ff = w_gate.shape[2]
        n_exp = w_gate.shape[0] * n_ep * n_nodes
        limit = max(1, min(top_k, n_nodes // 2))
        cap_node = min(tok_dev, 8 * ((5 * tok_dev * limit + 32 * n_nodes - 1) // (32 * n_nodes)))
        cap_exp = 8 * ((5 * n_nodes * tok_dev * top_k + 32 * n_exp - 1) // (32 * n_exp))
        n_chunks = cap_exp // BLK
        rows = n_ep * BLK

        cube = (SIDE, SIDE, SIDE, BLK, d_model)
        bf16, f32, i32 = jnp.bfloat16, jnp.float32, jnp.int32
        any_spec = pl.BlockSpec(memory_space=pl.ANY)
        dma = pltpu.SemaphoreType.DMA
        out, _, _ = pl.pallas_call(
            functools.partial(moe_kernel, n_chunks),
            name="moe_layer",
            out_shape=(jax.ShapeDtypeStruct((tok_dev, d_model), bf16),
                       jax.ShapeDtypeStruct((n_chunks,) + cube, bf16),
                       jax.ShapeDtypeStruct((n_chunks,) + cube, bf16)),
            in_specs=[any_spec] * 8,
            out_specs=(pl.BlockSpec(memory_space=pltpu.VMEM), any_spec, any_spec),
            scratch_shapes=[
                pltpu.VMEM((top_k, tok_dev), i32), pltpu.VMEM((top_k, tok_dev), f32),
                pltpu.VMEM((top_k, tok_dev), i32), pltpu.VMEM((top_k, tok_dev), i32),
                pltpu.VMEM((tok_dev, d_model), bf16),
                pltpu.VMEM((2, cap_node, tok_dev), bf16),
                *[pltpu.VMEM((SIDE, 2, cap_node, width), bf16) for _, width in part_columns(d_model)],
                pltpu.VMEM((2, top_k, tok_dev), f32), pltpu.VMEM((3, SIDE, 2, top_k, tok_dev), f32), pltpu.VMEM((top_k, tok_dev), f32),
                pltpu.VMEM((2, cap_node, 128), f32), pltpu.VMEM((cap_node, 128), f32),
                pltpu.VMEM((cap_node, d_model), bf16), pltpu.VMEM((cap_node, d_model), bf16),
                pltpu.VMEM((d_model, d_ff), bf16), pltpu.VMEM((d_model, d_ff), bf16), pltpu.VMEM((d_ff, d_model), bf16),
                pltpu.VMEM((2,) + cube, bf16),
                pltpu.VMEM((n_chunks,) + cube, bf16), pltpu.VMEM((n_chunks,) + cube, bf16), pltpu.VMEM((n_chunks,) + cube, bf16),
                pltpu.VMEM((rows, d_ff), bf16),
                pltpu.VMEM((2, cap_node, d_model), f32),
                dma((5,)), dma((3,)), dma((5, 2, 3)), dma((5, 2, 3, 3)), dma((5, n_chunks, 3, 3)), dma((6,)), dma((6,)),
                dma((3, 2, 2)), dma((3, 2, 2)), dma((3, 2, 2)), dma((3, 2, 2)), dma((3, 3)), dma((3, 3)),
            ],
            compiler_params=pltpu.CompilerParams(collective_id=0, has_side_effects=True, vmem_limit_bytes=63 * 2**20),
        )(expert_ids.T, route_w.T, node_slot.T, exp_slot.T, tokens, w_gate[0], w_up[0], w_down[0])
        return out

    return jax.shard_map(local_layer, mesh=mesh, in_specs=(row_spec,) * 5 + (exp_spec,) * 3, out_specs=row_spec, check_vma=False)
```

```python
import functools

import jax
import jax.numpy as jnp
from jax import lax
from jax.experimental import pallas as pl
from jax.experimental.pallas import tpu as pltpu
from jax.sharding import PartitionSpec as P

MESH = pl.DeviceIdType.MESH
SIDE = 4
SHIFTS = (1, 3, 2)
ROUTES = ((2, 1, 0), (1, 0, 2), (0, 2, 1))
STRIDE = (16, 4, 1)
BLK = 8
SLOTS = 64
NT = (((1,), (1,)), ((), ()))
TN = (((0,), (0,)), ((), ()))


def part_columns(d_model):
    tiles = d_model // 128
    base, extra = tiles // 3, tiles % 3
    cols, at = [], 0
    for k in range(3):
        width = (base + (1 if k >= 3 - extra else 0)) * 128
        cols.append((at, width))
        at += width
    return cols


def moe_kernel(n_chunks, ids_hbm, rw_hbm, ns_hbm, es_hbm, tok_hbm, wg_hbm, wu_hbm, wd_hbm, out_ref, mid_d, mid_r,
               ids, rw, ns, es, tok, pick, rg0, rg1, rg2, own_codes, codes, c_send, feat, f_send, p_buf, p_recv,
               wg, wu, wd, send1, hop, work, back, hid, acc, lhs,
               in_sem, w_sem, own_sem, send_sem, recv_sem, pair_send, pair_recv, a_send, a_recv, b_send, b_recv, c_ssem, c_rsem):
    f32, bf16 = jnp.float32, jnp.bfloat16
    tok_dev, d_model = tok_hbm.shape
    d_ff = wg_hbm.shape[1]
    top_k = ids_hbm.shape[0]
    n_ep = SIDE ** 3
    rows = n_ep * BLK
    cap = feat.shape[1]
    half = cap // 2
    node = lax.axis_index("node")
    other = 1 - node
    ep = lax.axis_index("ep")
    pos = (ep // (SIDE * SIDE), (ep // SIDE) % SIDE, ep % SIDE)
    cols = part_columns(d_model)
    rings = (rg0, rg1, rg2)

    def peer(dim, shift):
        at = [pos[0], pos[1], pos[2]]
        at[dim] = (pos[dim] + shift) % SIDE
        return (at[0] * SIDE + at[1]) * SIDE + at[2]

    def to_ep(src, dst, ssem, rsem, dim, shift):
        return pltpu.make_async_remote_copy(src_ref=src, dst_ref=dst, send_sem=ssem, recv_sem=rsem,
                                            device_id={"ep": peer(dim, shift)}, device_id_type=MESH)

    def to_pair(src, dst, i):
        return pltpu.make_async_remote_copy(src_ref=src, dst_ref=dst, send_sem=pair_send.at[i], recv_sem=pair_recv.at[i],
                                            device_id={"node": other}, device_id_type=MESH)

    inputs = [pltpu.make_async_copy(s, d, in_sem.at[i]) for i, (s, d) in enumerate(
        ((ids_hbm, ids), (rw_hbm, rw), (ns_hbm, ns), (es_hbm, es), (tok_hbm, tok)))]
    weights = [pltpu.make_async_copy(s, d, w_sem.at[i]) for i, (s, d) in enumerate(((wg_hbm, wg), (wu_hbm, wu), (wd_hbm, wd)))]
    for c in inputs:
        c.start()
    barrier = pltpu.get_barrier_semaphore()
    pl.semaphore_signal(barrier, inc=1, device_id={"node": other}, device_id_type=MESH)
    for dim in range(3):
        for shift in SHIFTS:
            pl.semaphore_signal(barrier, inc=1, device_id={"ep": peer(dim, shift)}, device_id_type=MESH)
    for c in inputs:
        c.wait()

    def on_group(m):
        return (ids[...] >= m * n_ep) & (ids[...] < (m + 1) * n_ep)

    def find_rows(m):
        slot = jnp.max(jnp.where(on_group(m), ns[...], -1), axis=0, keepdims=True)
        pick[m] = jnp.where(lax.broadcasted_iota(jnp.int32, (tok_dev, tok_dev), 0) == slot, 1.0, 0.0).astype(bf16)

    def route(m):
        kept = on_group(m) & (ns[...] >= 0) & (es[...] >= 0)
        a = jnp.where(kept, (ids[...] - m * n_ep) * SLOTS, 0).astype(f32)
        b = jnp.where(kept, es[...] + 1, 0).astype(f32)
        w = jnp.where(kept, rw[...], 0.0)
        w1 = w.astype(bf16).astype(f32)
        w2 = (w - w1).astype(bf16).astype(f32)
        w3 = w - w1 - w2
        fill = jnp.zeros((128 - 2 * top_k, tok_dev), f32)
        parts = [jnp.concatenate([p, q, fill], axis=0).astype(bf16) for p, q in ((a, w1), (b, w2), (jnp.zeros_like(a), w3))]
        code = sum(lax.dot_general(p, pick[m], NT, preferred_element_type=f32) for p in parts[:2])[:top_k]
        by_row = sum(lax.dot_general(pick[m, :cap], p, NT, preferred_element_type=f32) for p in parts[::-1])
        return code, by_row

    find_rows(node)
    for part in range(3):
        c0, width = cols[part]
        rings[part][pos[ROUTES[part][0]], node] = jnp.dot(
            pick[node, :cap], tok[:, c0:c0 + width], preferred_element_type=f32).astype(bf16)
    pl.semaphore_wait(barrier, 1 + 3 * len(SHIFTS))

    def ring_copies(part, n):
        dim, ring = ROUTES[part][0], rings[part]
        i = pos[dim]
        first = [to_ep(ring.at[i, n], ring.at[i, n], a_send.at[part, n, v], a_recv.at[part, n, v], dim, (1, 3)[v]) for v in range(2)]
        onward = []
        for v in range(2):
            k = (i + (3, 1)[v]) % SIDE
            span = pl.ds(v * half, half)
            onward.append(to_ep(ring.at[k, n, span], ring.at[k, n, span], b_send.at[part, n, v], b_recv.at[part, n, v], dim, (1, 3)[v]))
        return first, onward

    for part in range(3):
        for c in ring_copies(part, node)[0]:
            c.start()
    find_rows(other)
    p_buf[other] = jnp.dot(pick[other, :cap], tok[...], preferred_element_type=f32).astype(bf16)
    pair = [to_pair(p_buf.at[other, :, pl.ds(*cols[part])], rings[part].at[pos[ROUTES[part][0]], node], part) for part in range(3)]
    for c in pair:
        c.start()
    far_code, far_feat = route(other)
    c_send[...] = far_code
    f_send[...] = far_feat
    pair_codes = [to_pair(c_send, own_codes.at[node], 3), to_pair(f_send, feat.at[node], 4)]
    for c in pair_codes:
        c.start()
    own_code, own_feat = route(node)
    own_codes[node] = own_code
    feat[node] = own_feat
    for c in weights:
        c.start()
    acc[...] = jnp.zeros_like(acc)
    for c in pair:
        c.wait()
    for part in range(3):
        for c in ring_copies(part, other)[0]:
            c.start()
    for c in pair_codes:
        c.wait()
    code_copies = [to_ep(own_codes, codes.at[dim, pos[dim]], c_ssem.at[dim, v], c_rsem.at[dim, v], dim, shift)
                   for dim in range(3) for v, shift in enumerate(SHIFTS)]
    for c in code_copies:
        c.start()
    for dim in range(3):
        codes[dim, pos[dim]] = own_codes[...]
    for n in (node, other):
        for part in range(3):
            first, onward = ring_copies(part, n)
            for v in range(2):
                first[v].wait()
                onward[v].start()
    for c in code_copies:
        c.wait()

    stages = ((send1, mid_d, 1), (mid_d, work, 2), (work, hop, 2), (hop, mid_r, 1), (mid_r, back, 0))

    def plane(ref, chunk, dim, index, part):
        c0, width = cols[part]
        idx = [chunk, slice(None), slice(None), slice(None), slice(None), pl.ds(c0, width)]
        idx[1 + dim] = index
        return ref.at[tuple(idx)]

    def copies(stage, chunk):
        src, dst, leg = stages[stage]
        src_chunk = chunk % 2 if stage == 0 else chunk
        remote, local = [], []
        for part in range(3):
            dim = ROUTES[part][leg]
            for v, shift in enumerate(SHIFTS):
                remote.append(to_ep(plane(src, src_chunk, dim, (pos[dim] + shift) % SIDE, part),
                                    plane(dst, chunk, dim, pos[dim], part),
                                    send_sem.at[stage, chunk % 2, part, v], recv_sem.at[stage, chunk, part, v], dim, shift))
            local.append(pltpu.make_async_copy(
                plane(src, src_chunk, dim, pos[dim], part), plane(dst, chunk, dim, pos[dim], part),
                own_sem.at[stage, chunk % 2, part]))
        return remote, local

    def launch(stage, chunk):
        remote, local = copies(stage, chunk)
        for c in remote:
            c.start()
        for c in local:
            c.start()

    def finish(stage, chunk):
        remote, local = copies(stage, chunk)
        for c in remote:
            c.wait()
        for c in local:
            c.wait()

    def first_leg(chunk, part, k):
        ring, dim = ROUTES[part][0], ROUTES[part][1]
        c0, width = cols[part]

        def line(ref, slot, index):
            idx = [slot, slice(None), slice(None), slice(None), slice(None), pl.ds(c0, width)]
            idx[1 + ring], idx[1 + dim] = k, index
            return ref.at[tuple(idx)]

        for v, shift in enumerate(SHIFTS):
            to_ep(line(send1, chunk % 2, (pos[dim] + shift) % SIDE), line(mid_d, chunk, pos[dim]),
                  send_sem.at[0, chunk % 2, part, v], recv_sem.at[0, chunk, part, v], dim, shift).start()
        pltpu.make_async_copy(line(send1, chunk % 2, pos[dim]), line(mid_d, chunk, pos[dim]), own_sem.at[0, chunk % 2, part]).start()

    def gather(chunk):
        for v in (0, 3, 1, 2):
            for part in range(3):
                if v == 2:
                    @pl.when(chunk == 0)
                    def _():
                        for n in (node, other):
                            for c in ring_copies(part, n)[1]:
                                c.wait()
                dim = ROUTES[part][0]
                k = (pos[dim] + v) % SIDE
                c0, width = cols[part]
                o0, o1 = [d for d in range(3) if d != dim]
                r = lax.broadcasted_iota(jnp.int32, (SIDE * SIDE * BLK, cap), 0)
                expert = pos[dim] * STRIDE[dim] + (r >> 5) * STRIDE[o0] + ((r >> 3) & 3) * STRIDE[o1]
                want = (expert * SLOTS + (r & 7) + chunk * BLK + 1).astype(f32)
                block = None
                for n in range(2):
                    hit = jnp.zeros(want.shape, f32)
                    for j in range(top_k):
                        hit = jnp.where(codes[dim, k, n, j:j + 1, :cap] == want, 1.0, hit)
                    got = jnp.dot(hit.astype(bf16), rings[part][k, n], preferred_element_type=f32)
                    block = got if block is None else block + got
                idx = [chunk % 2, slice(None), slice(None), slice(None), slice(None), slice(c0, c0 + width)]
                idx[1 + dim] = k
                send1[tuple(idx)] = block.reshape(SIDE, SIDE, BLK, width).astype(bf16)
                first_leg(chunk, part, k)

    def ffn(chunk):
        width = 256

        def up(n, carry):
            at = pl.ds(pl.multiple_of(n * width, width), width)
            x = work[chunk].reshape(rows, d_model)
            g = jnp.dot(x, wg[:, at], preferred_element_type=f32)
            u = jnp.dot(x, wu[:, at], preferred_element_type=f32)
            hid[:, at] = (jax.nn.silu(g) * u).astype(bf16)
            return carry

        lax.fori_loop(0, d_ff // width, up, 0)

        def down(n, carry):
            at = pl.ds(pl.multiple_of(n * width, width), width)
            y = jnp.dot(hid[...], wd[:, at], preferred_element_type=f32)
            work[chunk, :, :, :, :, at] = y.reshape(SIDE, SIDE, SIDE, BLK, width).astype(bf16)
            return carry

        lax.fori_loop(0, d_model // width, down, 0)

    def mix(chunk):
        lane = lax.broadcasted_iota(jnp.int32, (cap, rows), 1)
        want = ((lane >> 3) * SLOTS + (lane & 7) + chunk * BLK + 1).astype(f32)
        for n in range(2):
            w = jnp.zeros((cap, rows), f32)
            for j in range(top_k):
                w = jnp.where(feat[n, :, j:j + 1] == want, feat[n, :, top_k + j:top_k + j + 1], w)
            hi = w.astype(bf16)
            rest = w - hi.astype(f32)
            mid = rest.astype(bf16)
            lo = (rest - mid.astype(f32)).astype(bf16)
            for i, term in enumerate((lo, mid, hi)):
                lhs[(2 * i + n) * cap:(2 * i + n + 1) * cap, :] = term

    def mixed(chunk, at):
        y = back[chunk, :, :, :, :, at].reshape(rows, at.stop - at.start)
        add = jnp.dot(lhs[...], y, preferred_element_type=f32)
        return acc[:, at] + (add[:2 * cap] + add[2 * cap:4 * cap] + add[4 * cap:])

    spans = [slice(q, q + 512) for q in range(0, d_model, 512)]

    def step(t, carry):
        @pl.when(t < n_chunks)
        def _():
            gather(t)

        for stage in range(1, 6):
            chunk = t - stage

            @pl.when((chunk >= 0) & (chunk < (n_chunks if stage < 5 else n_chunks - 1)))
            def _():
                if stage == 5:
                    mix(chunk)
                finish(stage - 1, chunk)
                if stage == 2:
                    @pl.when(chunk == 0)
                    def _():
                        for c in weights:
                            c.wait()
                    ffn(chunk)
                if stage < 5:
                    launch(stage, chunk)
                else:
                    for at in spans:
                        acc[:, at] = mixed(chunk, at)
        return carry

    lax.fori_loop(0, n_chunks + 4, step, 0)

    last = n_chunks - 1
    mix(last)
    finish(4, last)
    share = []
    for i, at in enumerate(spans):
        p_buf[:, :, at] = mixed(last, at).reshape(2, cap, at.stop - at.start).astype(bf16)
        share.append(to_pair(p_buf.at[other, :, pl.ds(at.start, at.stop - at.start)], p_recv.at[:, pl.ds(at.start, at.stop - at.start)], 5 + i))
        share[-1].start()
    for c, at in zip(share, spans):
        mine = lax.dot_general(pick[node, :cap], p_buf[node, :, at], TN, preferred_element_type=f32)
        c.wait()
        theirs = lax.dot_general(pick[other, :cap], p_recv[:, at], TN, preferred_element_type=f32)
        out_ref[:, at] = (mine + theirs).astype(bf16)


def solution(mesh):
    n_nodes = mesh.shape['node']
    n_ep = mesh.shape['ep']
    row_spec = P(('dp', 'node', 'ep'), None)
    exp_spec = P(('node', 'ep'), None, None)

    def local_layer(tokens, expert_ids, route_w, node_slot, exp_slot, w_gate, w_up, w_down):
        tok_dev, d_model = tokens.shape
        top_k = expert_ids.shape[1]
        d_ff = w_gate.shape[2]
        n_exp = w_gate.shape[0] * n_ep * n_nodes
        limit = max(1, min(top_k, n_nodes // 2))
        cap_node = min(tok_dev, 8 * ((5 * tok_dev * limit + 32 * n_nodes - 1) // (32 * n_nodes)))
        cap_exp = 8 * ((5 * n_nodes * tok_dev * top_k + 32 * n_exp - 1) // (32 * n_exp))
        n_chunks = cap_exp // BLK
        rows = n_ep * BLK

        cube = (SIDE, SIDE, SIDE, BLK, d_model)
        bf16, f32, i32 = jnp.bfloat16, jnp.float32, jnp.int32
        any_spec = pl.BlockSpec(memory_space=pl.ANY)
        dma = pltpu.SemaphoreType.DMA
        out, _, _ = pl.pallas_call(
            functools.partial(moe_kernel, n_chunks),
            name="moe_layer",
            out_shape=(jax.ShapeDtypeStruct((tok_dev, d_model), bf16),
                       jax.ShapeDtypeStruct((n_chunks,) + cube, bf16),
                       jax.ShapeDtypeStruct((n_chunks,) + cube, bf16)),
            in_specs=[any_spec] * 8,
            out_specs=(pl.BlockSpec(memory_space=pltpu.VMEM), any_spec, any_spec),
            scratch_shapes=[
                pltpu.VMEM((top_k, tok_dev), i32), pltpu.VMEM((top_k, tok_dev), f32),
                pltpu.VMEM((top_k, tok_dev), i32), pltpu.VMEM((top_k, tok_dev), i32),
                pltpu.VMEM((tok_dev, d_model), bf16),
                pltpu.VMEM((2, tok_dev, tok_dev), bf16),
                *[pltpu.VMEM((SIDE, 2, cap_node, width), bf16) for _, width in part_columns(d_model)],
                pltpu.VMEM((2, top_k, tok_dev), f32), pltpu.VMEM((3, SIDE, 2, top_k, tok_dev), f32), pltpu.VMEM((top_k, tok_dev), f32),
                pltpu.VMEM((2, cap_node, 128), f32), pltpu.VMEM((cap_node, 128), f32),
                pltpu.VMEM((2, cap_node, d_model), bf16), pltpu.VMEM((cap_node, d_model), bf16),
                pltpu.VMEM((d_model, d_ff), bf16), pltpu.VMEM((d_model, d_ff), bf16), pltpu.VMEM((d_ff, d_model), bf16),
                pltpu.VMEM((2,) + cube, bf16),
                pltpu.VMEM((n_chunks,) + cube, bf16), pltpu.VMEM((n_chunks,) + cube, bf16), pltpu.VMEM((n_chunks,) + cube, bf16),
                pltpu.VMEM((rows, d_ff), bf16),
                pltpu.VMEM((2 * cap_node, d_model), f32),
                pltpu.VMEM((6 * cap_node, rows), bf16),
                dma((5,)), dma((3,)), dma((5, 2, 3)), dma((5, 2, 3, 3)), dma((5, n_chunks, 3, 3)), dma((9,)), dma((9,)),
                dma((3, 2, 2)), dma((3, 2, 2)), dma((3, 2, 2)), dma((3, 2, 2)), dma((3, 3)), dma((3, 3)),
            ],
            compiler_params=pltpu.CompilerParams(collective_id=0, has_side_effects=True, vmem_limit_bytes=63 * 2**20),
        )(expert_ids.T, route_w.T, node_slot.T, exp_slot.T, tokens, w_gate[0], w_up[0], w_down[0])
        return out

    return jax.shard_map(local_layer, mesh=mesh, in_specs=(row_spec,) * 5 + (exp_spec,) * 3, out_specs=row_spec, check_vma=False)
```

```python
import functools

import jax
import jax.numpy as jnp
from jax import lax
from jax.experimental import pallas as pl
from jax.experimental.pallas import tpu as pltpu
from jax.sharding import PartitionSpec as P

MESH = pl.DeviceIdType.MESH
SIDE = 4
SHIFTS = (1, 3, 2)
ROUTES = ((2, 1, 0), (1, 0, 2), (0, 2, 1))
STRIDE = (16, 4, 1)
BLK = 8
SLOTS = 64
NT = (((1,), (1,)), ((), ()))
TN = (((0,), (0,)), ((), ()))


def part_columns(d_model):
    tiles = d_model // 128
    base, extra = tiles // 3, tiles % 3
    cols, at = [], 0
    for k in range(3):
        width = (base + (1 if k >= 3 - extra else 0)) * 128
        cols.append((at, width))
        at += width
    return cols


def moe_kernel(n_chunks, ids_hbm, rw_hbm, ns_hbm, es_hbm, tok_hbm, wg_hbm, wu_hbm, wd_hbm, out_ref, mid_d, hop,
               ids, rw, ns, es, tok, pick, rg0, rg1, rg2, own_codes, codes, c_send, p_buf, p_recv,
               wg, wu, wd, send1, work, mid_r, hid, acc0, acc1, acc2, far0, far1, far2, near0, near1, near2,
               in_sem, w_sem, own_sem, send_sem, recv_sem, pair_send, pair_recv, a_send, a_recv, b_send, b_recv, c_ssem, c_rsem,
               f_send, f_recv, n_send, n_recv):
    f32, bf16 = jnp.float32, jnp.bfloat16
    tok_dev, d_model = tok_hbm.shape
    d_ff = wg_hbm.shape[1]
    top_k = ids_hbm.shape[0]
    n_ep = SIDE ** 3
    rows = n_ep * BLK
    cap = p_recv.shape[0]
    half = cap // 2
    node = lax.axis_index("node")
    other = 1 - node
    ep = lax.axis_index("ep")
    pos = (ep // (SIDE * SIDE), (ep // SIDE) % SIDE, ep % SIDE)
    cols = part_columns(d_model)
    rings, accs, fars, nears = (rg0, rg1, rg2), (acc0, acc1, acc2), (far0, far1, far2), (near0, near1, near2)

    def peer(dim, shift):
        at = [pos[0], pos[1], pos[2]]
        at[dim] = (pos[dim] + shift) % SIDE
        return (at[0] * SIDE + at[1]) * SIDE + at[2]

    def to_ep(src, dst, ssem, rsem, dim, shift):
        return pltpu.make_async_remote_copy(src_ref=src, dst_ref=dst, send_sem=ssem, recv_sem=rsem,
                                            device_id={"ep": peer(dim, shift)}, device_id_type=MESH)

    def to_pair(src, dst, i):
        return pltpu.make_async_remote_copy(src_ref=src, dst_ref=dst, send_sem=pair_send.at[i], recv_sem=pair_recv.at[i],
                                            device_id={"node": other}, device_id_type=MESH)

    inputs = [pltpu.make_async_copy(s, d, in_sem.at[i]) for i, (s, d) in enumerate(
        ((ids_hbm, ids), (rw_hbm, rw), (ns_hbm, ns), (es_hbm, es), (tok_hbm, tok)))]
    weights = [pltpu.make_async_copy(s, d, w_sem.at[i]) for i, (s, d) in enumerate(((wg_hbm, wg), (wu_hbm, wu), (wd_hbm, wd)))]
    for c in inputs:
        c.start()
    barrier = pltpu.get_barrier_semaphore()
    pl.semaphore_signal(barrier, inc=1, device_id={"node": other}, device_id_type=MESH)
    for dim in range(3):
        for shift in SHIFTS:
            pl.semaphore_signal(barrier, inc=1, device_id={"ep": peer(dim, shift)}, device_id_type=MESH)
    for c in inputs:
        c.wait()

    def on_group(m):
        return (ids[...] >= m * n_ep) & (ids[...] < (m + 1) * n_ep)

    def find_rows(m):
        slot = jnp.max(jnp.where(on_group(m), ns[...], -1), axis=0, keepdims=True)
        pick[m] = jnp.where(lax.broadcasted_iota(jnp.int32, (tok_dev, tok_dev), 0) == slot, 1.0, 0.0).astype(bf16)

    def route(m):
        kept = on_group(m) & (ns[...] >= 0) & (es[...] >= 0)
        a = jnp.where(kept, (ids[...] - m * n_ep) * SLOTS, 0).astype(f32)
        b = jnp.where(kept, es[...] + 1, 0).astype(f32)
        w = jnp.where(kept, rw[...], 0.0)
        w1 = w.astype(bf16).astype(f32)
        w2 = (w - w1).astype(bf16).astype(f32)
        w3 = w - w1 - w2
        parts = [jnp.concatenate([p, q], axis=0).astype(bf16) for p, q in ((a, w1), (b, w2), (jnp.zeros_like(a), w3))]
        return sum(lax.dot_general(p, pick[m], NT, preferred_element_type=f32) for p in parts[::-1])

    find_rows(node)
    for part in range(3):
        c0, width = cols[part]
        rings[part][pos[ROUTES[part][0]], node] = jnp.dot(
            pick[node, :cap], tok[:, c0:c0 + width], preferred_element_type=f32).astype(bf16)
    pl.semaphore_wait(barrier, 1 + 3 * len(SHIFTS))

    def ring_copies(part, n):
        dim, ring = ROUTES[part][0], rings[part]
        i = pos[dim]
        first = [to_ep(ring.at[i, n], ring.at[i, n], a_send.at[part, n, v], a_recv.at[part, n, v], dim, (1, 3)[v]) for v in range(2)]
        onward = []
        for v in range(2):
            k = (i + (3, 1)[v]) % SIDE
            span = pl.ds(v * half, half)
            onward.append(to_ep(ring.at[k, n, span], ring.at[k, n, span], b_send.at[part, n, v], b_recv.at[part, n, v], dim, (1, 3)[v]))
        return first, onward

    for part in range(3):
        for c in ring_copies(part, node)[0]:
            c.start()
    find_rows(other)
    p_buf[other] = jnp.dot(pick[other, :cap], tok[...], preferred_element_type=f32).astype(bf16)
    pair = [to_pair(p_buf.at[other, :, pl.ds(*cols[part])], rings[part].at[pos[ROUTES[part][0]], node], part) for part in range(3)]
    for c in pair:
        c.start()
    c_send[...] = route(other)
    pair_codes = to_pair(c_send, own_codes.at[node], 3)
    pair_codes.start()
    own_codes[node] = route(node)
    for c in weights:
        c.start()
    for acc in accs:
        acc[...] = jnp.zeros_like(acc)
    for c in pair:
        c.wait()
    for part in range(3):
        for c in ring_copies(part, other)[0]:
            c.start()
    pair_codes.wait()
    code_copies = [to_ep(own_codes, codes.at[dim, pos[dim]], c_ssem.at[dim, v], c_rsem.at[dim, v], dim, shift)
                   for dim in range(3) for v, shift in enumerate(SHIFTS)]
    for c in code_copies:
        c.start()
    for dim in range(3):
        codes[dim, pos[dim]] = own_codes[...]
    for n in (node, other):
        for part in range(3):
            first, onward = ring_copies(part, n)
            for v in range(2):
                first[v].wait()
                onward[v].start()
    for c in code_copies:
        c.wait()

    stages = ((send1, mid_d, 1), (mid_d, work, 2), (work, hop, 2), (hop, mid_r, 1))

    def plane(ref, chunk, dim, index, part):
        c0, width = cols[part]
        idx = [chunk, slice(None), slice(None), slice(None), slice(None), pl.ds(c0, width)]
        idx[1 + dim] = index
        return ref.at[tuple(idx)]

    def copies(stage, chunk):
        src, dst, leg = stages[stage]
        src_chunk = chunk % 2 if stage == 0 else chunk
        remote, local = [], []
        for part in range(3):
            dim = ROUTES[part][leg]
            for v, shift in enumerate(SHIFTS):
                remote.append(to_ep(plane(src, src_chunk, dim, (pos[dim] + shift) % SIDE, part),
                                    plane(dst, chunk, dim, pos[dim], part),
                                    send_sem.at[stage, chunk % 2, part, v], recv_sem.at[stage, chunk, part, v], dim, shift))
            local.append(pltpu.make_async_copy(
                plane(src, src_chunk, dim, pos[dim], part), plane(dst, chunk, dim, pos[dim], part),
                own_sem.at[stage, chunk % 2, part]))
        return remote, local

    def launch(stage, chunk):
        remote, local = copies(stage, chunk)
        for c in remote:
            c.start()
        for c in local:
            c.start()

    def finish(stage, chunk):
        remote, local = copies(stage, chunk)
        for c in remote:
            c.wait()
        for c in local:
            c.wait()

    def first_leg(chunk, part, k):
        ring, dim = ROUTES[part][0], ROUTES[part][1]
        c0, width = cols[part]

        def line(ref, slot, index):
            idx = [slot, slice(None), slice(None), slice(None), slice(None), pl.ds(c0, width)]
            idx[1 + ring], idx[1 + dim] = k, index
            return ref.at[tuple(idx)]

        for v, shift in enumerate(SHIFTS):
            to_ep(line(send1, chunk % 2, (pos[dim] + shift) % SIDE), line(mid_d, chunk, pos[dim]),
                  send_sem.at[0, chunk % 2, part, v], recv_sem.at[0, chunk, part, v], dim, shift).start()
        pltpu.make_async_copy(line(send1, chunk % 2, pos[dim]), line(mid_d, chunk, pos[dim]), own_sem.at[0, chunk % 2, part]).start()

    def plane_codes(chunk, dim):
        o0, o1 = [d for d in range(3) if d != dim]
        r = lax.broadcasted_iota(jnp.int32, (SIDE * SIDE * BLK, cap), 0)
        expert = pos[dim] * STRIDE[dim] + (r >> 5) * STRIDE[o0] + ((r >> 3) & 3) * STRIDE[o1]
        return (expert * SLOTS + (r & 7) + chunk * BLK + 1).astype(f32)

    def gather(chunk):
        for v in (0, 3, 1, 2):
            for part in range(3):
                if v == 2:
                    @pl.when(chunk == 0)
                    def _():
                        for n in (node, other):
                            for c in ring_copies(part, n)[1]:
                                c.wait()
                dim = ROUTES[part][0]
                k = (pos[dim] + v) % SIDE
                c0, width = cols[part]
                want = plane_codes(chunk, dim)
                block = None
                for n in range(2):
                    hit = jnp.zeros(want.shape, f32)
                    for j in range(top_k):
                        hit = jnp.where(codes[dim, k, n, j:j + 1, :cap] == want, 1.0, hit)
                    got = jnp.dot(hit.astype(bf16), rings[part][k, n], preferred_element_type=f32)
                    block = got if block is None else block + got
                idx = [chunk % 2, slice(None), slice(None), slice(None), slice(None), slice(c0, c0 + width)]
                idx[1 + dim] = k
                send1[tuple(idx)] = block.reshape(SIDE, SIDE, BLK, width).astype(bf16)
                first_leg(chunk, part, k)

    def ffn(chunk):
        width = 256

        def up(n, carry):
            at = pl.ds(pl.multiple_of(n * width, width), width)
            x = work[chunk].reshape(rows, d_model)
            g = jnp.dot(x, wg[:, at], preferred_element_type=f32)
            u = jnp.dot(x, wu[:, at], preferred_element_type=f32)
            hid[:, at] = (jax.nn.silu(g) * u).astype(bf16)
            return carry

        lax.fori_loop(0, d_ff // width, up, 0)

        def down(n, carry):
            at = pl.ds(pl.multiple_of(n * width, width), width)
            y = jnp.dot(hid[...], wd[:, at], preferred_element_type=f32)
            work[chunk, :, :, :, :, at] = y.reshape(SIDE, SIDE, SIDE, BLK, width).astype(bf16)
            return carry

        lax.fori_loop(0, d_model // width, down, 0)

    def fold(chunk, v, part):
        dim = ROUTES[part][0]
        k = (pos[dim] + v) % SIDE
        c0, width = cols[part]
        want = plane_codes(chunk, dim)
        idx = [chunk, slice(None), slice(None), slice(None), slice(None), slice(c0, c0 + width)]
        idx[1 + dim] = k
        y = mid_r[tuple(idx)].reshape(SIDE * SIDE * BLK, width)
        y = jnp.concatenate([y, y, y], axis=0)
        for n in range(2):
            w = jnp.zeros(want.shape, f32)
            for j in range(top_k):
                w = jnp.where(codes[dim, k, n, j:j + 1, :cap] == want, codes[dim, k, n, top_k + j:top_k + j + 1, :cap], w)
            hi = w.astype(bf16)
            rest = w - hi.astype(f32)
            mid = rest.astype(bf16)
            lo = (rest - mid.astype(f32)).astype(bf16)
            terms = jnp.concatenate([lo, mid, hi], axis=0)
            accs[part][k, n] += lax.dot_general(terms, y, TN, preferred_element_type=f32)

    def step(t, carry):
        @pl.when(t < n_chunks)
        def _():
            gather(t)

        for stage in range(1, 5):
            chunk = t - stage

            @pl.when((chunk >= 0) & (chunk < (n_chunks if stage < 4 else n_chunks - 1)))
            def _():
                finish(stage - 1, chunk)
                if stage == 2:
                    @pl.when(chunk == 0)
                    def _():
                        for c in weights:
                            c.wait()
                    ffn(chunk)
                if stage < 4:
                    launch(stage, chunk)
                else:
                    for v in range(SIDE):
                        for part in range(3):
                            fold(chunk, v, part)
        return carry

    lax.fori_loop(0, n_chunks + 3, step, 0)

    def far_copies(part, n):
        dim = ROUTES[part][0]
        k = (pos[dim] + 2) % SIDE
        return [to_ep(accs[part].at[k, n, pl.ds(v * half, half)], fars[part].at[v, n], f_send.at[part, n, v], f_recv.at[part, n, v],
                      dim, (1, 3)[v]) for v in range(2)]

    def near_copies(part, n):
        dim = ROUTES[part][0]
        return [to_ep(accs[part].at[(pos[dim] + (1, 3)[v]) % SIDE, n], nears[part].at[v, n], n_send.at[part, n, v], n_recv.at[part, n, v],
                      dim, (1, 3)[v]) for v in range(2)]

    last = n_chunks - 1
    finish(3, last)
    for part in range(3):
        fold(last, 2, part)
        for c in far_copies(part, other):
            c.start()
    for part in range(3):
        for c in far_copies(part, node):
            c.start()
    for v in (1, 3, 0):
        for part in range(3):
            fold(last, v, part)
    for n in (other, node):
        for part in range(3):
            i = pos[ROUTES[part][0]]
            for v, c in enumerate(far_copies(part, n)):
                c.wait()
                accs[part][(i + (1, 3)[v]) % SIDE, n, v * half:(v + 1) * half] += fars[part][v, n]
            for c in near_copies(part, n):
                c.start()

    def total(part, n):
        for c in near_copies(part, n):
            c.wait()
        return (accs[part][pos[ROUTES[part][0]], n] + nears[part][0, n] + nears[part][1, n]).astype(bf16)

    spans = [slice(c0, c0 + width) for c0, width in cols]
    share = []
    for part, at in enumerate(spans):
        p_buf[other, :, at] = total(part, other)
        share.append(to_pair(p_buf.at[other, :, pl.ds(*cols[part])], p_recv.at[:, pl.ds(*cols[part])], 4 + part))
        share[-1].start()
    for c in share:
        c.wait()
    for at in spans:
        out_ref[:, at] = lax.dot_general(pick[other, :cap], p_recv[:, at], TN, preferred_element_type=f32).astype(bf16)
    for part, at in enumerate(spans):
        mine = lax.dot_general(pick[node, :cap], total(part, node), TN, preferred_element_type=f32)
        out_ref[:, at] = (out_ref[:, at].astype(f32) + mine).astype(bf16)


def solution(mesh):
    n_nodes = mesh.shape['node']
    n_ep = mesh.shape['ep']
    row_spec = P(('dp', 'node', 'ep'), None)
    exp_spec = P(('node', 'ep'), None, None)

    def local_layer(tokens, expert_ids, route_w, node_slot, exp_slot, w_gate, w_up, w_down):
        tok_dev, d_model = tokens.shape
        top_k = expert_ids.shape[1]
        d_ff = w_gate.shape[2]
        n_exp = w_gate.shape[0] * n_ep * n_nodes
        limit = max(1, min(top_k, n_nodes // 2))
        cap_node = min(tok_dev, 8 * ((5 * tok_dev * limit + 32 * n_nodes - 1) // (32 * n_nodes)))
        cap_exp = 8 * ((5 * n_nodes * tok_dev * top_k + 32 * n_exp - 1) // (32 * n_exp))
        n_chunks = cap_exp // BLK
        rows = n_ep * BLK

        cube = (SIDE, SIDE, SIDE, BLK, d_model)
        bf16, f32, i32 = jnp.bfloat16, jnp.float32, jnp.int32
        any_spec = pl.BlockSpec(memory_space=pl.ANY)
        dma = pltpu.SemaphoreType.DMA
        out, _, _ = pl.pallas_call(
            functools.partial(moe_kernel, n_chunks),
            name="moe_layer",
            out_shape=(jax.ShapeDtypeStruct((tok_dev, d_model), bf16),
                       jax.ShapeDtypeStruct((n_chunks,) + cube, bf16),
                       jax.ShapeDtypeStruct((n_chunks,) + cube, bf16)),
            in_specs=[any_spec] * 8,
            out_specs=(pl.BlockSpec(memory_space=pltpu.VMEM), any_spec, any_spec),
            scratch_shapes=[
                pltpu.VMEM((top_k, tok_dev), i32), pltpu.VMEM((top_k, tok_dev), f32),
                pltpu.VMEM((top_k, tok_dev), i32), pltpu.VMEM((top_k, tok_dev), i32),
                pltpu.VMEM((tok_dev, d_model), bf16),
                pltpu.VMEM((2, tok_dev, tok_dev), bf16),
                *[pltpu.VMEM((SIDE, 2, cap_node, width), bf16) for _, width in part_columns(d_model)],
                pltpu.VMEM((2, 2 * top_k, tok_dev), f32), pltpu.VMEM((3, SIDE, 2, 2 * top_k, tok_dev), f32), pltpu.VMEM((2 * top_k, tok_dev), f32),
                pltpu.VMEM((2, cap_node, d_model), bf16), pltpu.VMEM((cap_node, d_model), bf16),
                pltpu.VMEM((d_model, d_ff), bf16), pltpu.VMEM((d_model, d_ff), bf16), pltpu.VMEM((d_ff, d_model), bf16),
                pltpu.VMEM((2,) + cube, bf16), pltpu.VMEM((n_chunks,) + cube, bf16), pltpu.VMEM((n_chunks,) + cube, bf16),
                pltpu.VMEM((rows, d_ff), bf16),
                *[pltpu.VMEM((SIDE, 2, cap_node, width), f32) for _, width in part_columns(d_model)],
                *[pltpu.VMEM((2, 2, cap_node // 2, width), f32) for _, width in part_columns(d_model)],
                *[pltpu.VMEM((2, 2, cap_node, width), f32) for _, width in part_columns(d_model)],
                dma((5,)), dma((3,)), dma((4, 2, 3)), dma((4, 2, 3, 3)), dma((4, n_chunks, 3, 3)), dma((7,)), dma((7,)),
                dma((3, 2, 2)), dma((3, 2, 2)), dma((3, 2, 2)), dma((3, 2, 2)), dma((3, 3)), dma((3, 3)),
                dma((3, 2, 2)), dma((3, 2, 2)), dma((3, 2, 2)), dma((3, 2, 2)),
            ],
            compiler_params=pltpu.CompilerParams(collective_id=0, has_side_effects=True, vmem_limit_bytes=67_043_328),
        )(expert_ids.T, route_w.T, node_slot.T, exp_slot.T, tokens, w_gate[0], w_up[0], w_down[0])
        return out

    return jax.shard_map(local_layer, mesh=mesh, in_specs=(row_spec,) * 5 + (exp_spec,) * 3, out_specs=row_spec, check_vma=False)
```

```python
import functools

import jax
import jax.numpy as jnp
from jax import lax
from jax.experimental import pallas as pl
from jax.experimental.pallas import tpu as pltpu
from jax.sharding import PartitionSpec as P

MESH = pl.DeviceIdType.MESH
SIDE = 4
SHIFTS = (1, 3, 2)
ROUTES = ((2, 1, 0), (1, 0, 2), (0, 2, 1))
STRIDE = (16, 4, 1)
BLK = 8
SLOTS = 64
NT = (((1,), (1,)), ((), ()))
TN = (((0,), (0,)), ((), ()))


def part_columns(d_model):
    width = d_model // 128 // 3 * 128
    return [(k * width, width) for k in range(3)]


def moe_kernel(n_chunks, ids_hbm, rw_hbm, ns_hbm, es_hbm, tok_hbm, wg_hbm, wu_hbm, wd_hbm, out_ref, mid_d, hop,
               ids, rw, ns, es, tok, pick, rg0, rg1, rg2, own_codes, codes, c_send, p_buf, p_recv, x_rows, x_send, x_leg, x_back, x_acc,
               wg, wu, wd, send1, work, mid_r, hid, acc0, acc1, acc2, far0, far1, far2, near0, near1, near2,
               in_sem, w_sem, own_sem, send_sem, recv_sem, pair_send, pair_recv, a_send, a_recv, b_send, b_recv, c_ssem, c_rsem,
               f_send, f_recv, n_send, n_recv, x_ssem, x_rsem, x_osem):
    f32, bf16 = jnp.float32, jnp.bfloat16
    tok_dev, d_model = tok_hbm.shape
    d_ff = wg_hbm.shape[1]
    top_k = ids_hbm.shape[0]
    n_ep = SIDE ** 3
    rows = n_ep * BLK
    cap = p_recv.shape[0]
    half = cap // 2
    node = lax.axis_index("node")
    other = 1 - node
    ep = lax.axis_index("ep")
    pos = (ep // (SIDE * SIDE), (ep // SIDE) % SIDE, ep % SIDE)
    cols = part_columns(d_model)
    rest = cols[2][0] + cols[2][1]
    rings, accs, fars, nears = (rg0, rg1, rg2), (acc0, acc1, acc2), (far0, far1, far2), (near0, near1, near2)

    def peer(dim, shift):
        at = [pos[0], pos[1], pos[2]]
        at[dim] = (pos[dim] + shift) % SIDE
        return (at[0] * SIDE + at[1]) * SIDE + at[2]

    def to_ep(src, dst, ssem, rsem, dim, shift):
        return pltpu.make_async_remote_copy(src_ref=src, dst_ref=dst, send_sem=ssem, recv_sem=rsem,
                                            device_id={"ep": peer(dim, shift)}, device_id_type=MESH)

    def to_pair(src, dst, i):
        return pltpu.make_async_remote_copy(src_ref=src, dst_ref=dst, send_sem=pair_send.at[i], recv_sem=pair_recv.at[i],
                                            device_id={"node": other}, device_id_type=MESH)

    inputs = [pltpu.make_async_copy(s, d, in_sem.at[i]) for i, (s, d) in enumerate(
        ((ids_hbm, ids), (rw_hbm, rw), (ns_hbm, ns), (es_hbm, es), (tok_hbm, tok)))]
    weights = [pltpu.make_async_copy(s, d, w_sem.at[i]) for i, (s, d) in enumerate(((wg_hbm, wg), (wu_hbm, wu), (wd_hbm, wd)))]
    for c in inputs:
        c.start()
    barrier = pltpu.get_barrier_semaphore()
    pl.semaphore_signal(barrier, inc=1, device_id={"node": other}, device_id_type=MESH)
    for dim in range(3):
        for shift in SHIFTS:
            pl.semaphore_signal(barrier, inc=1, device_id={"ep": peer(dim, shift)}, device_id_type=MESH)
    for c in inputs:
        c.wait()

    def on_group(m):
        return (ids[...] >= m * n_ep) & (ids[...] < (m + 1) * n_ep)

    def find_rows(m):
        slot = jnp.max(jnp.where(on_group(m), ns[...], -1), axis=0, keepdims=True)
        pick[m] = jnp.where(lax.broadcasted_iota(jnp.int32, (tok_dev, tok_dev), 0) == slot, 1.0, 0.0).astype(bf16)

    def route(m):
        kept = on_group(m) & (ns[...] >= 0) & (es[...] >= 0)
        a = jnp.where(kept, (ids[...] - m * n_ep) * SLOTS, 0).astype(f32)
        b = jnp.where(kept, es[...] + 1, 0).astype(f32)
        w = jnp.where(kept, rw[...], 0.0)
        w1 = w.astype(bf16).astype(f32)
        w2 = (w - w1).astype(bf16).astype(f32)
        w3 = w - w1 - w2
        parts = [jnp.concatenate([p, q], axis=0).astype(bf16) for p, q in ((a, w1), (b, w2), (jnp.zeros_like(a), w3))]
        return sum(lax.dot_general(p, pick[m], NT, preferred_element_type=f32) for p in parts[::-1])

    find_rows(node)
    for part in range(3):
        c0, width = cols[part]
        rings[part][pos[ROUTES[part][0]], node] = jnp.dot(
            pick[node, :cap], tok[:, c0:c0 + width], preferred_element_type=f32).astype(bf16)
    x_rows[node] = jnp.dot(pick[node, :cap], tok[:, rest:], preferred_element_type=f32).astype(bf16)
    pl.semaphore_wait(barrier, 1 + 3 * len(SHIFTS))

    def ring_copies(part, n):
        dim, ring = ROUTES[part][0], rings[part]
        i = pos[dim]
        first = [to_ep(ring.at[i, n], ring.at[i, n], a_send.at[part, n, v], a_recv.at[part, n, v], dim, (1, 3)[v]) for v in range(2)]
        onward = []
        for v in range(2):
            k = (i + (3, 1)[v]) % SIDE
            span = pl.ds(v * half, half)
            onward.append(to_ep(ring.at[k, n, span], ring.at[k, n, span], b_send.at[part, n, v], b_recv.at[part, n, v], dim, (1, 3)[v]))
        return first, onward

    for part in range(3):
        for c in ring_copies(part, node)[0]:
            c.start()
    find_rows(other)
    p_buf[other] = jnp.dot(pick[other, :cap], tok[...], preferred_element_type=f32).astype(bf16)
    pair = [to_pair(p_buf.at[other, :, pl.ds(*cols[part])], rings[part].at[pos[ROUTES[part][0]], node], part) for part in range(3)]
    pair.append(to_pair(p_buf.at[other, :, pl.ds(rest, d_model - rest)], x_rows.at[node], 7))
    for c in pair:
        c.start()
    c_send[...] = route(other)
    pair_codes = to_pair(c_send, own_codes.at[node], 3)
    pair_codes.start()
    own_codes[node] = route(node)
    for c in weights:
        c.start()
    for acc in accs:
        acc[...] = jnp.zeros_like(acc)
    for c in pair:
        c.wait()
    for part in range(3):
        for c in ring_copies(part, other)[0]:
            c.start()
    pair_codes.wait()
    code_copies = [to_ep(own_codes, codes.at[dim, pos[dim]], c_ssem.at[dim, v], c_rsem.at[dim, v], dim, shift)
                   for dim in range(3) for v, shift in enumerate(SHIFTS)]
    for c in code_copies:
        c.start()
    for dim in range(3):
        codes[dim, pos[dim]] = own_codes[...]
    stages = ((send1, mid_d, 1), (mid_d, work, 2), (work, hop, 2), (hop, mid_r, 1))

    def plane(ref, chunk, dim, index, part):
        c0, width = cols[part]
        idx = [chunk, slice(None), slice(None), slice(None), slice(None), pl.ds(c0, width)]
        idx[1 + dim] = index
        return ref.at[tuple(idx)]

    def copies(stage, chunk):
        src, dst, leg = stages[stage]
        src_chunk = chunk % 2 if stage == 0 else chunk
        remote, local = [], []
        for part in range(3):
            dim = ROUTES[part][leg]
            for v, shift in enumerate(SHIFTS):
                remote.append(to_ep(plane(src, src_chunk, dim, (pos[dim] + shift) % SIDE, part),
                                    plane(dst, chunk, dim, pos[dim], part),
                                    send_sem.at[stage, chunk % 2, part, v], recv_sem.at[stage, chunk, part, v], dim, shift))
            local.append(pltpu.make_async_copy(
                plane(src, src_chunk, dim, pos[dim], part), plane(dst, chunk, dim, pos[dim], part),
                own_sem.at[stage, chunk % 2, part]))
        return remote, local

    def launch(stage, chunk):
        remote, local = copies(stage, chunk)
        for c in remote:
            c.start()
        for c in local:
            c.start()

    def finish(stage, chunk):
        remote, local = copies(stage, chunk)
        for c in remote:
            c.wait()
        for c in local:
            c.wait()

    def plane_codes(chunk, dim, at):
        o0, o1 = [d for d in range(3) if d != dim]
        r = lax.broadcasted_iota(jnp.int32, (SIDE * SIDE * BLK, cap), 0)
        expert = at * STRIDE[dim] + (r >> 5) * STRIDE[o0] + ((r >> 3) & 3) * STRIDE[o1]
        return (expert * SLOTS + (r & 7) + chunk * BLK + 1).astype(f32)

    def pick_slots(want, code, packed):
        block = None
        for n in range(2):
            hit = jnp.zeros(want.shape, f32)
            for j in range(top_k):
                hit = jnp.where(code[n, j:j + 1, :cap] == want, 1.0, hit)
            got = jnp.dot(hit.astype(bf16), packed[n], preferred_element_type=f32)
            block = got if block is None else block + got
        return block.astype(bf16).reshape(SIDE, SIDE, BLK, -1)

    def weigh_slots(want, code, y, n):
        w = jnp.zeros(want.shape, f32)
        for j in range(top_k):
            w = jnp.where(code[n, j:j + 1, :cap] == want, code[n, top_k + j:top_k + j + 1, :cap], w)
        hi = w.astype(bf16)
        left = w - hi.astype(f32)
        mid = left.astype(bf16)
        lo = (left - mid.astype(f32)).astype(bf16)
        return lax.dot_general(jnp.concatenate([lo, mid, hi], axis=0), jnp.concatenate([y, y, y], axis=0), TN, preferred_element_type=f32)

    x_stages = ((x_send, x_leg), (x_leg, mid_d), (mid_d, work), (work, hop), (hop, mid_r), (mid_r, x_back))

    def x_copies(leg, chunk, route_no):
        src, dst = x_stages[leg]
        dim = ROUTES[route_no][leg if leg < 3 else 5 - leg]

        def at(ref, index):
            c0 = 0 if ref.shape[-1] == d_model - rest else rest
            idx = [chunk % 2 if ref is x_send else chunk, slice(None), slice(None), slice(None), slice(None), pl.ds(c0, d_model - rest)]
            idx[1 + dim] = index
            return ref.at[tuple(idx)]

        remote = [to_ep(at(src, (pos[dim] + shift) % SIDE), at(dst, pos[dim]), x_ssem.at[leg, chunk % 2, v], x_rsem.at[leg, chunk, v], dim, shift)
                  for v, shift in enumerate(SHIFTS)]
        return remote + [pltpu.make_async_copy(at(src, pos[dim]), at(dst, pos[dim]), x_osem.at[leg, chunk % 2])]

    def x_launch(leg, chunk):
        for route_no in range(3):
            @pl.when(chunk % 3 == route_no)
            def _():
                for c in x_copies(leg, chunk, route_no):
                    c.start()

    def x_finish(leg, chunk):
        for route_no in range(3):
            @pl.when(chunk % 3 == route_no)
            def _():
                for c in x_copies(leg, chunk, route_no):
                    c.wait()

    def x_gather(chunk):
        for z in range(SIDE):
            x_send[chunk % 2, z] = pick_slots(plane_codes(chunk, 0, z), own_codes, x_rows)
        x_launch(0, chunk)

    def x_combine(chunk):
        x_finish(5, chunk)
        for z in range(SIDE):
            y = x_back[chunk, z].reshape(SIDE * SIDE * BLK, d_model - rest)
            want = plane_codes(chunk, 0, z)
            for n in range(2):
                x_acc[n] += weigh_slots(want, own_codes, y, n)

    x_acc[...] = jnp.zeros_like(x_acc)
    x_gather(0)
    for n in (node, other):
        for part in range(3):
            first, onward = ring_copies(part, n)
            for v in range(2):
                first[v].wait()
                onward[v].start()
    for c in code_copies:
        c.wait()

    def first_leg(chunk, part, k):
        ring, dim = ROUTES[part][0], ROUTES[part][1]
        c0, width = cols[part]

        def line(ref, slot, index):
            idx = [slot, slice(None), slice(None), slice(None), slice(None), pl.ds(c0, width)]
            idx[1 + ring], idx[1 + dim] = k, index
            return ref.at[tuple(idx)]

        for v, shift in enumerate(SHIFTS):
            to_ep(line(send1, chunk % 2, (pos[dim] + shift) % SIDE), line(mid_d, chunk, pos[dim]),
                  send_sem.at[0, chunk % 2, part, v], recv_sem.at[0, chunk, part, v], dim, shift).start()
        pltpu.make_async_copy(line(send1, chunk % 2, pos[dim]), line(mid_d, chunk, pos[dim]), own_sem.at[0, chunk % 2, part]).start()

    def gather(chunk):
        for v in (0, 3, 1, 2):
            for part in range(3):
                if v == 2:
                    @pl.when(chunk == 0)
                    def _():
                        for n in (node, other):
                            for c in ring_copies(part, n)[1]:
                                c.wait()
                dim = ROUTES[part][0]
                k = (pos[dim] + v) % SIDE
                c0, width = cols[part]
                idx = [chunk % 2, slice(None), slice(None), slice(None), slice(None), slice(c0, c0 + width)]
                idx[1 + dim] = k
                send1[tuple(idx)] = pick_slots(plane_codes(chunk, dim, pos[dim]), codes.at[dim, k], rings[part].at[k])
                first_leg(chunk, part, k)

    def ffn(chunk):
        width = 256

        def up(n, carry):
            at = pl.ds(pl.multiple_of(n * width, width), width)
            x = work[chunk].reshape(rows, d_model)
            g = jnp.dot(x, wg[:, at], preferred_element_type=f32)
            u = jnp.dot(x, wu[:, at], preferred_element_type=f32)
            hid[:, at] = (jax.nn.silu(g) * u).astype(bf16)
            return carry

        lax.fori_loop(0, d_ff // width, up, 0)

        def down(n, carry):
            at = pl.ds(pl.multiple_of(n * width, width), width)
            y = jnp.dot(hid[...], wd[:, at], preferred_element_type=f32)
            work[chunk, :, :, :, :, at] = y.reshape(SIDE, SIDE, SIDE, BLK, width).astype(bf16)
            return carry

        lax.fori_loop(0, d_model // width, down, 0)

    def fold(chunk, v, part):
        dim = ROUTES[part][0]
        k = (pos[dim] + v) % SIDE
        c0, width = cols[part]
        want = plane_codes(chunk, dim, pos[dim])
        idx = [chunk, slice(None), slice(None), slice(None), slice(None), slice(c0, c0 + width)]
        idx[1 + dim] = k
        y = mid_r[tuple(idx)].reshape(SIDE * SIDE * BLK, width)
        for n in range(2):
            accs[part][k, n] += weigh_slots(want, codes.at[dim, k], y, n)

    def step(t, carry):
        @pl.when(t < n_chunks)
        def _():
            gather(t)
            x_finish(0, t)
            x_launch(1, t)

        @pl.when(t + 1 < n_chunks)
        def _():
            x_gather(t + 1)

        for stage in range(1, 5):
            chunk = t - stage

            @pl.when((chunk >= 0) & (chunk < (n_chunks if stage < 4 else n_chunks - 1)))
            def _():
                finish(stage - 1, chunk)
                x_finish(stage, chunk)
                if stage == 2:
                    @pl.when(chunk == 0)
                    def _():
                        for c in weights:
                            c.wait()
                    ffn(chunk)
                x_launch(stage + 1, chunk)
                if stage < 4:
                    launch(stage, chunk)
                else:
                    for v in range(SIDE):
                        for part in range(3):
                            fold(chunk, v, part)

        @pl.when(t >= 5)
        def _():
            x_combine(t - 5)

        return carry

    lax.fori_loop(0, n_chunks + 3, step, 0)

    def far_copies(part, n):
        dim = ROUTES[part][0]
        k = (pos[dim] + 2) % SIDE
        return [to_ep(accs[part].at[k, n, pl.ds(v * half, half)], fars[part].at[v, n], f_send.at[part, n, v], f_recv.at[part, n, v],
                      dim, (1, 3)[v]) for v in range(2)]

    def near_copies(part, n):
        dim = ROUTES[part][0]
        return [to_ep(accs[part].at[(pos[dim] + (1, 3)[v]) % SIDE, n], nears[part].at[v, n], n_send.at[part, n, v], n_recv.at[part, n, v],
                      dim, (1, 3)[v]) for v in range(2)]

    last = n_chunks - 1
    finish(3, last)
    for part in range(3):
        fold(last, 2, part)
        for c in far_copies(part, other):
            c.start()
    for part in range(3):
        for c in far_copies(part, node):
            c.start()
    x_finish(4, last)
    x_launch(5, last)
    for v in (1, 3, 0):
        for part in range(3):
            fold(last, v, part)
    for n in (other, node):
        for part in range(3):
            i = pos[ROUTES[part][0]]
            for v, c in enumerate(far_copies(part, n)):
                c.wait()
                accs[part][(i + (1, 3)[v]) % SIDE, n, v * half:(v + 1) * half] += fars[part][v, n]
            for c in near_copies(part, n):
                c.start()

    for chunk in range(max(n_chunks - 2, 0), n_chunks):
        x_combine(chunk)

    def total(part, n):
        for c in near_copies(part, n):
            c.wait()
        return (accs[part][pos[ROUTES[part][0]], n] + nears[part][0, n] + nears[part][1, n]).astype(bf16)

    spans = [slice(c0, c0 + width) for c0, width in cols]
    share = []
    for part, at in enumerate(spans):
        p_buf[other, :, at] = total(part, other)
        share.append(to_pair(p_buf.at[other, :, pl.ds(*cols[part])], p_recv.at[:, pl.ds(*cols[part])], 4 + part))
        share[-1].start()
    p_buf[other, :, rest:] = x_acc[other].astype(bf16)
    share.append(to_pair(p_buf.at[other, :, pl.ds(rest, d_model - rest)], p_recv.at[:, pl.ds(rest, d_model - rest)], 8))
    share[-1].start()
    for c in share:
        c.wait()
    x_sum = lax.dot_general(pick[other, :cap], p_recv[:, rest:], TN, preferred_element_type=f32)
    x_sum = x_sum + lax.dot_general(pick[node, :cap], x_acc[node].astype(bf16), TN, preferred_element_type=f32)
    out_ref[:, rest:] = x_sum.astype(bf16)
    for at in spans:
        out_ref[:, at] = lax.dot_general(pick[other, :cap], p_recv[:, at], TN, preferred_element_type=f32).astype(bf16)
    for part, at in enumerate(spans):
        mine = lax.dot_general(pick[node, :cap], total(part, node), TN, preferred_element_type=f32)
        out_ref[:, at] = (out_ref[:, at].astype(f32) + mine).astype(bf16)


def solution(mesh):
    n_nodes = mesh.shape['node']
    n_ep = mesh.shape['ep']
    row_spec = P(('dp', 'node', 'ep'), None)
    exp_spec = P(('node', 'ep'), None, None)

    def local_layer(tokens, expert_ids, route_w, node_slot, exp_slot, w_gate, w_up, w_down):
        tok_dev, d_model = tokens.shape
        top_k = expert_ids.shape[1]
        d_ff = w_gate.shape[2]
        n_exp = w_gate.shape[0] * n_ep * n_nodes
        limit = max(1, min(top_k, n_nodes // 2))
        cap_node = min(tok_dev, 8 * ((5 * tok_dev * limit + 32 * n_nodes - 1) // (32 * n_nodes)))
        cap_exp = 8 * ((5 * n_nodes * tok_dev * top_k + 32 * n_exp - 1) // (32 * n_exp))
        n_chunks = cap_exp // BLK
        rows = n_ep * BLK

        cube = (SIDE, SIDE, SIDE, BLK, d_model)
        wide = d_model - 3 * part_columns(d_model)[0][1]
        x_cube = (SIDE, SIDE, SIDE, BLK, wide)
        bf16, f32, i32 = jnp.bfloat16, jnp.float32, jnp.int32
        any_spec = pl.BlockSpec(memory_space=pl.ANY)
        dma = pltpu.SemaphoreType.DMA
        out, _, _ = pl.pallas_call(
            functools.partial(moe_kernel, n_chunks),
            name="moe_layer",
            out_shape=(jax.ShapeDtypeStruct((tok_dev, d_model), bf16),
                       jax.ShapeDtypeStruct((n_chunks,) + cube, bf16),
                       jax.ShapeDtypeStruct((n_chunks,) + cube, bf16)),
            in_specs=[any_spec] * 8,
            out_specs=(pl.BlockSpec(memory_space=pltpu.VMEM), any_spec, any_spec),
            scratch_shapes=[
                pltpu.VMEM((top_k, tok_dev), i32), pltpu.VMEM((top_k, tok_dev), f32),
                pltpu.VMEM((top_k, tok_dev), i32), pltpu.VMEM((top_k, tok_dev), i32),
                pltpu.VMEM((tok_dev, d_model), bf16),
                pltpu.VMEM((2, tok_dev, tok_dev), bf16),
                *[pltpu.VMEM((SIDE, 2, cap_node, width), bf16) for _, width in part_columns(d_model)],
                pltpu.VMEM((2, 2 * top_k, tok_dev), f32), pltpu.VMEM((3, SIDE, 2, 2 * top_k, tok_dev), f32), pltpu.VMEM((2 * top_k, tok_dev), f32),
                pltpu.VMEM((2, cap_node, d_model), bf16), pltpu.VMEM((cap_node, d_model), bf16),
                pltpu.VMEM((2, cap_node, wide), bf16), pltpu.VMEM((2,) + x_cube, bf16), pltpu.VMEM((n_chunks,) + x_cube, bf16),
                pltpu.VMEM((n_chunks,) + x_cube, bf16), pltpu.VMEM((2, cap_node, wide), f32),
                pltpu.VMEM((d_model, d_ff), bf16), pltpu.VMEM((d_model, d_ff), bf16), pltpu.VMEM((d_ff, d_model), bf16),
                pltpu.VMEM((2,) + cube, bf16), pltpu.VMEM((n_chunks,) + cube, bf16), pltpu.VMEM((n_chunks,) + cube, bf16),
                pltpu.VMEM((rows, d_ff), bf16),
                *[pltpu.VMEM((SIDE, 2, cap_node, width), f32) for _, width in part_columns(d_model)],
                *[pltpu.VMEM((2, 2, cap_node // 2, width), f32) for _, width in part_columns(d_model)],
                *[pltpu.VMEM((2, 2, cap_node, width), f32) for _, width in part_columns(d_model)],
                dma((5,)), dma((3,)), dma((4, 2, 3)), dma((4, 2, 3, 3)), dma((4, n_chunks, 3, 3)), dma((9,)), dma((9,)),
                dma((3, 2, 2)), dma((3, 2, 2)), dma((3, 2, 2)), dma((3, 2, 2)), dma((3, 3)), dma((3, 3)),
                dma((3, 2, 2)), dma((3, 2, 2)), dma((3, 2, 2)), dma((3, 2, 2)),
                dma((6, 2, 3)), dma((6, n_chunks, 3)), dma((6, 2)),
            ],
            compiler_params=pltpu.CompilerParams(collective_id=0, has_side_effects=True, vmem_limit_bytes=67_043_328),
        )(expert_ids.T, route_w.T, node_slot.T, exp_slot.T, tokens, w_gate[0], w_up[0], w_down[0])
        return out

    return jax.shard_map(local_layer, mesh=mesh, in_specs=(row_spec,) * 5 + (exp_spec,) * 3, out_specs=row_spec, check_vma=False)
```

```python
import functools

import jax
import jax.numpy as jnp
from jax import lax
from jax.experimental import pallas as pl
from jax.experimental.pallas import tpu as pltpu
from jax.sharding import PartitionSpec as P

MESH = pl.DeviceIdType.MESH
SIDE = 4
SHIFTS = (1, 3, 2)
ROUTES = ((2, 1, 0), (1, 0, 2), (0, 2, 1))
STRIDE = (16, 4, 1)
BLK = 8
SLOTS = 64
NT = (((1,), (1,)), ((), ()))
TN = (((0,), (0,)), ((), ()))


def part_columns(d_model):
    width = d_model // 128 // 3 * 128
    return [(k * width, width) for k in range(3)]


def moe_kernel(n_chunks, ids_hbm, rw_hbm, ns_hbm, es_hbm, tok_hbm, wg_hbm, wu_hbm, wd_hbm, out_ref, mid_d, hop,
               ids, rw, ns, es, tok, pick, rg0, rg1, rg2, own_codes, codes, c_send, p_buf, p_recv, x_rows, x_send, x_leg, x_back, x_acc,
               wg, wu, wd, send1, work, mid_r, hid, acc0, acc1, acc2, far0, far1, far2, near0, near1, near2,
               in_sem, w_sem, own_sem, send_sem, recv_sem, pair_send, pair_recv, a_send, a_recv, b_send, b_recv, c_ssem, c_rsem,
               f_send, f_recv, n_send, n_recv, x_ssem, x_rsem, x_osem, l_send, l_recv, l_own, o_sem):
    f32, bf16 = jnp.float32, jnp.bfloat16
    tok_dev, d_model = tok_hbm.shape
    d_ff = wg_hbm.shape[1]
    top_k = ids_hbm.shape[0]
    n_ep = SIDE ** 3
    rows = n_ep * BLK
    cap = p_recv.shape[0]
    half = cap // 2
    node = lax.axis_index("node")
    other = 1 - node
    ep = lax.axis_index("ep")
    pos = (ep // (SIDE * SIDE), (ep // SIDE) % SIDE, ep % SIDE)
    cols = part_columns(d_model)
    rest = cols[2][0] + cols[2][1]
    rings, accs, fars, nears = (rg0, rg1, rg2), (acc0, acc1, acc2), (far0, far1, far2), (near0, near1, near2)

    def peer(dim, shift):
        at = [pos[0], pos[1], pos[2]]
        at[dim] = (pos[dim] + shift) % SIDE
        return (at[0] * SIDE + at[1]) * SIDE + at[2]

    def to_ep(src, dst, ssem, rsem, dim, shift):
        return pltpu.make_async_remote_copy(src_ref=src, dst_ref=dst, send_sem=ssem, recv_sem=rsem,
                                            device_id={"ep": peer(dim, shift)}, device_id_type=MESH)

    def to_pair(src, dst, i):
        return pltpu.make_async_remote_copy(src_ref=src, dst_ref=dst, send_sem=pair_send.at[i], recv_sem=pair_recv.at[i],
                                            device_id={"node": other}, device_id_type=MESH)

    inputs = [pltpu.make_async_copy(s, d, in_sem.at[i]) for i, (s, d) in enumerate(
        ((ids_hbm, ids), (rw_hbm, rw), (ns_hbm, ns), (es_hbm, es), (tok_hbm, tok)))]
    weights = [pltpu.make_async_copy(s, d, w_sem.at[i]) for i, (s, d) in enumerate(((wg_hbm, wg), (wu_hbm, wu), (wd_hbm, wd)))]
    for c in inputs:
        c.start()
    barrier = pltpu.get_barrier_semaphore()
    pl.semaphore_signal(barrier, inc=1, device_id={"node": other}, device_id_type=MESH)
    for dim in range(3):
        for shift in SHIFTS:
            pl.semaphore_signal(barrier, inc=1, device_id={"ep": peer(dim, shift)}, device_id_type=MESH)
    for c in inputs:
        c.wait()

    def on_group(m):
        return (ids[...] >= m * n_ep) & (ids[...] < (m + 1) * n_ep)

    def find_rows(m):
        slot = jnp.max(jnp.where(on_group(m), ns[...], -1), axis=0, keepdims=True)
        pick[m] = jnp.where(lax.broadcasted_iota(jnp.int32, (tok_dev, tok_dev), 0) == slot, 1.0, 0.0).astype(bf16)

    def route(m):
        kept = on_group(m) & (ns[...] >= 0) & (es[...] >= 0)
        a = jnp.where(kept, (ids[...] - m * n_ep) * SLOTS, 0).astype(f32)
        b = jnp.where(kept, es[...] + 1, 0).astype(f32)
        w = jnp.where(kept, rw[...], 0.0)
        w1 = w.astype(bf16).astype(f32)
        w2 = (w - w1).astype(bf16).astype(f32)
        w3 = w - w1 - w2
        parts = [jnp.concatenate([p, q], axis=0).astype(bf16) for p, q in ((a, w1), (b, w2), (jnp.zeros_like(a), w3))]
        return sum(lax.dot_general(p, pick[m], NT, preferred_element_type=f32) for p in parts[::-1])

    find_rows(node)
    for part in range(3):
        c0, width = cols[part]
        rings[part][pos[ROUTES[part][0]], node] = jnp.dot(
            pick[node, :cap], tok[:, c0:c0 + width], preferred_element_type=f32).astype(bf16)
    x_rows[node] = jnp.dot(pick[node, :cap], tok[:, rest:], preferred_element_type=f32).astype(bf16)
    pl.semaphore_wait(barrier, 1 + 3 * len(SHIFTS))

    def ring_copies(part, n):
        dim, ring = ROUTES[part][0], rings[part]
        i = pos[dim]
        first = [to_ep(ring.at[i, n], ring.at[i, n], a_send.at[part, n, v], a_recv.at[part, n, v], dim, (1, 3)[v]) for v in range(2)]
        onward = []
        for v in range(2):
            k = (i + (3, 1)[v]) % SIDE
            span = pl.ds(v * half, half)
            onward.append(to_ep(ring.at[k, n, span], ring.at[k, n, span], b_send.at[part, n, v], b_recv.at[part, n, v], dim, (1, 3)[v]))
        return first, onward

    for part in range(3):
        for c in ring_copies(part, node)[0]:
            c.start()
    find_rows(other)
    p_buf[other] = jnp.dot(pick[other, :cap], tok[...], preferred_element_type=f32).astype(bf16)
    pair = [to_pair(p_buf.at[other, :, pl.ds(*cols[part])], rings[part].at[pos[ROUTES[part][0]], node], part) for part in range(3)]
    pair.append(to_pair(p_buf.at[other, :, pl.ds(rest, d_model - rest)], x_rows.at[node], 7))
    for c in pair:
        c.start()
    c_send[...] = route(other)
    pair_codes = to_pair(c_send, own_codes.at[node], 3)
    pair_codes.start()
    own_codes[node] = route(node)
    for c in weights:
        c.start()
    for acc in accs:
        acc[...] = jnp.zeros_like(acc)
    for c in pair:
        c.wait()
    for part in range(3):
        for c in ring_copies(part, other)[0]:
            c.start()
    pair_codes.wait()
    code_copies = [to_ep(own_codes, codes.at[dim, pos[dim]], c_ssem.at[dim, v], c_rsem.at[dim, v], dim, shift)
                   for dim in range(3) for v, shift in enumerate(SHIFTS)]
    for c in code_copies:
        c.start()
    for dim in range(3):
        codes[dim, pos[dim]] = own_codes[...]
    stages = ((send1, mid_d, 1), (mid_d, work, 2), (work, hop, 2), (hop, mid_r, 1))

    def plane(ref, chunk, dim, index, part):
        c0, width = cols[part]
        idx = [chunk, slice(None), slice(None), slice(None), slice(None), pl.ds(c0, width)]
        idx[1 + dim] = index
        return ref.at[tuple(idx)]

    def copies(stage, chunk):
        src, dst, leg = stages[stage]
        src_chunk = chunk % 2 if stage == 0 else chunk
        remote, local = [], []
        for part in range(3):
            dim = ROUTES[part][leg]
            for v, shift in enumerate(SHIFTS):
                remote.append(to_ep(plane(src, src_chunk, dim, (pos[dim] + shift) % SIDE, part),
                                    plane(dst, chunk, dim, pos[dim], part),
                                    send_sem.at[stage, chunk % 2, part, v], recv_sem.at[stage, chunk, part, v], dim, shift))
            local.append(pltpu.make_async_copy(
                plane(src, src_chunk, dim, pos[dim], part), plane(dst, chunk, dim, pos[dim], part),
                own_sem.at[stage, chunk % 2, part]))
        return remote, local

    def launch(stage, chunk):
        remote, local = copies(stage, chunk)
        for c in remote:
            c.start()
        for c in local:
            c.start()

    def finish(stage, chunk):
        remote, local = copies(stage, chunk)
        for c in remote:
            c.wait()
        for c in local:
            c.wait()

    def plane_codes(chunk, dim, at):
        o0, o1 = [d for d in range(3) if d != dim]
        r = lax.broadcasted_iota(jnp.int32, (SIDE * SIDE * BLK, cap), 0)
        expert = at * STRIDE[dim] + (r >> 5) * STRIDE[o0] + ((r >> 3) & 3) * STRIDE[o1]
        return (expert * SLOTS + (r & 7) + chunk * BLK + 1).astype(f32)

    def pick_slots(want, code, packed):
        block = None
        for n in range(2):
            hit = jnp.zeros(want.shape, f32)
            for j in range(top_k):
                hit = jnp.where(code[n, j:j + 1, :cap] == want, 1.0, hit)
            got = jnp.dot(hit.astype(bf16), packed[n], preferred_element_type=f32)
            block = got if block is None else block + got
        return block.astype(bf16).reshape(SIDE, SIDE, BLK, -1)

    def weigh_slots(want, code, y, n):
        w = jnp.zeros(want.shape, f32)
        for j in range(top_k):
            w = jnp.where(code[n, j:j + 1, :cap] == want, code[n, top_k + j:top_k + j + 1, :cap], w)
        hi = w.astype(bf16)
        left = w - hi.astype(f32)
        mid = left.astype(bf16)
        lo = (left - mid.astype(f32)).astype(bf16)
        return lax.dot_general(jnp.concatenate([lo, mid, hi], axis=0), jnp.concatenate([y, y, y], axis=0), TN, preferred_element_type=f32)

    x_stages = ((x_send, x_leg), (x_leg, mid_d), (mid_d, work), (work, hop), (hop, mid_r), (mid_r, x_back))

    def x_copies(leg, chunk, route_no):
        src, dst = x_stages[leg]
        dim = ROUTES[route_no][leg if leg < 3 else 5 - leg]

        def at(ref, index):
            c0 = 0 if ref.shape[-1] == d_model - rest else rest
            idx = [chunk % 2 if ref is x_send else chunk, slice(None), slice(None), slice(None), slice(None), pl.ds(c0, d_model - rest)]
            idx[1 + dim] = index
            return ref.at[tuple(idx)]

        remote = [to_ep(at(src, (pos[dim] + shift) % SIDE), at(dst, pos[dim]), x_ssem.at[leg, chunk, v], x_rsem.at[leg, chunk, v], dim, shift)
                  for v, shift in enumerate(SHIFTS)]
        return remote + [pltpu.make_async_copy(at(src, pos[dim]), at(dst, pos[dim]), x_osem.at[leg, chunk])]

    def x_launch(leg, chunk):
        for route_no in range(3):
            @pl.when(chunk % 3 == route_no)
            def _():
                for c in x_copies(leg, chunk, route_no):
                    c.start()

    def x_finish(leg, chunk):
        for route_no in range(3):
            @pl.when(chunk % 3 == route_no)
            def _():
                for c in x_copies(leg, chunk, route_no):
                    c.wait()

    def x_gather(chunk):
        def pick_plane(z, carry):
            x_send[chunk % 2, z] = pick_slots(plane_codes(chunk, 0, z), own_codes, x_rows)
            return carry

        lax.fori_loop(0, SIDE, pick_plane, 0)
        x_launch(0, chunk)

    def x_combine(chunk):
        x_finish(5, chunk)

        def add_plane(z, carry):
            y = x_back[chunk, z].reshape(SIDE * SIDE * BLK, d_model - rest)
            want = plane_codes(chunk, 0, z)
            for n in range(2):
                x_acc[n] += weigh_slots(want, own_codes, y, n)
            return carry

        lax.fori_loop(0, SIDE, add_plane, 0)

    x_acc[...] = jnp.zeros_like(x_acc)
    x_gather(0)
    for n in (node, other):
        for part in range(3):
            first, onward = ring_copies(part, n)
            for v in range(2):
                first[v].wait()
                onward[v].start()
    for c in code_copies:
        c.wait()

    def line(ref, slot, part, k, index):
        idx = [slot, slice(None), slice(None), slice(None), slice(None), pl.ds(*cols[part])]
        idx[1 + ROUTES[part][0]], idx[1 + ROUTES[part][1]] = k, index
        return ref.at[tuple(idx)]

    def first_leg(chunk, part, k):
        dim = ROUTES[part][1]
        for v, shift in enumerate(SHIFTS):
            to_ep(line(send1, chunk % 2, part, k, (pos[dim] + shift) % SIDE), line(mid_d, chunk, part, k, pos[dim]),
                  send_sem.at[0, chunk % 2, part, v], recv_sem.at[0, chunk, part, v], dim, shift).start()
        pltpu.make_async_copy(line(send1, chunk % 2, part, k, pos[dim]), line(mid_d, chunk, part, k, pos[dim]),
                              own_sem.at[0, chunk % 2, part]).start()

    def last_leg(chunk, part, v):
        dim = ROUTES[part][1]
        k = (pos[ROUTES[part][0]] + v) % SIDE
        made = [to_ep(line(hop, chunk, part, k, (pos[dim] + shift) % SIDE), line(mid_r, chunk, part, k, pos[dim]),
                      l_send.at[v, part, i], l_recv.at[v, part, i], dim, shift) for i, shift in enumerate(SHIFTS)]
        return made + [pltpu.make_async_copy(line(hop, chunk, part, k, pos[dim]), line(mid_r, chunk, part, k, pos[dim]), l_own.at[v, part])]

    def gather(chunk):
        for v in (0, 3, 1, 2):
            for part in range(3):
                if v == 2:
                    @pl.when(chunk == 0)
                    def _():
                        for n in (node, other):
                            for c in ring_copies(part, n)[1]:
                                c.wait()
                dim = ROUTES[part][0]
                k = (pos[dim] + v) % SIDE
                c0, width = cols[part]
                idx = [chunk % 2, slice(None), slice(None), slice(None), slice(None), slice(c0, c0 + width)]
                idx[1 + dim] = k
                send1[tuple(idx)] = pick_slots(plane_codes(chunk, dim, pos[dim]), codes.at[dim, k], rings[part].at[k])
                first_leg(chunk, part, k)

    def ffn(chunk):
        width = 256

        def up(n, carry):
            at = pl.ds(pl.multiple_of(n * width, width), width)
            x = work[chunk].reshape(rows, d_model)
            g = jnp.dot(x, wg[:, at], preferred_element_type=f32)
            u = jnp.dot(x, wu[:, at], preferred_element_type=f32)
            hid[:, at] = (jax.nn.silu(g) * u).astype(bf16)
            return carry

        lax.fori_loop(0, d_ff // width, up, 0)

        def down(n, carry):
            at = pl.ds(pl.multiple_of(n * width, width), width)
            y = jnp.dot(hid[...], wd[:, at], preferred_element_type=f32)
            work[chunk, :, :, :, :, at] = y.reshape(SIDE, SIDE, SIDE, BLK, width).astype(bf16)
            return carry

        lax.fori_loop(0, d_model // width, down, 0)

    def fold(chunk, v, part):
        dim = ROUTES[part][0]
        k = (pos[dim] + v) % SIDE
        c0, width = cols[part]
        want = plane_codes(chunk, dim, pos[dim])
        idx = [chunk, slice(None), slice(None), slice(None), slice(None), slice(c0, c0 + width)]
        idx[1 + dim] = k
        y = mid_r[tuple(idx)].reshape(SIDE * SIDE * BLK, width)
        for n in range(2):
            accs[part][k, n] += weigh_slots(want, codes.at[dim, k], y, n)

    def step(t, carry):
        @pl.when(t < n_chunks)
        def _():
            gather(t)
            x_finish(0, t)
            x_launch(1, t)

        @pl.when(t + 1 < n_chunks)
        def _():
            x_gather(t + 1)

        for stage in range(1, 5):
            chunk = t - stage

            @pl.when((chunk >= 0) & (chunk < (n_chunks if stage < 4 else n_chunks - 1)))
            def _():
                finish(stage - 1, chunk)
                x_finish(stage, chunk)
                if stage == 2:
                    @pl.when(chunk == 0)
                    def _():
                        for c in weights:
                            c.wait()
                    ffn(chunk)
                x_launch(stage + 1, chunk)
                if stage < 4:
                    launch(stage, chunk)
                else:
                    def fold_source(v, carry):
                        for part in range(3):
                            fold(chunk, v, part)
                        return carry

                    lax.fori_loop(0, SIDE, fold_source, 0)

        @pl.when(t >= 5)
        def _():
            x_combine(t - 5)

        return carry

    lax.fori_loop(0, n_chunks + 2, step, 0)

    def far_copies(part, n):
        dim = ROUTES[part][0]
        k = (pos[dim] + 2) % SIDE
        return [to_ep(accs[part].at[k, n, pl.ds(v * half, half)], fars[part].at[v, n], f_send.at[part, n, v], f_recv.at[part, n, v],
                      dim, (1, 3)[v]) for v in range(2)]

    first = (cols[0][1] // 128 + 1) // 2 * 128
    pieces = ((0, first), (first, cols[0][1] - first))

    def near_copies(part, n, piece):
        dim = ROUTES[part][0]
        span = pl.ds(*pieces[piece])
        return [to_ep(accs[part].at[(pos[dim] + (1, 3)[v]) % SIDE, n, :, span], nears[part].at[v, n, :, span],
                      n_send.at[part, n, piece, v], n_recv.at[part, n, piece, v], dim, (1, 3)[v]) for v in range(2)]

    last, prev = n_chunks - 1, n_chunks - 2

    finish(2, last)
    x_finish(3, last)

    def start_source(i, carry):
        for part in range(3):
            for c in last_leg(last, part, (2 + 3 * i) % SIDE):
                c.start()
        return carry

    lax.fori_loop(0, SIDE, start_source, 0)
    x_launch(4, last)
    finish(3, prev)
    x_finish(4, prev)
    x_launch(5, prev)

    def fold_far(i, carry):
        for part in range(3):
            @pl.when(i == 1)
            def _():
                for c in last_leg(last, part, 2):
                    c.wait()
            fold(prev + i, 2, part)

            @pl.when(i == 1)
            def _():
                for c in far_copies(part, other):
                    c.start()
        return carry

    lax.fori_loop(0, 2, fold_far, 0)
    for part in range(3):
        for c in far_copies(part, node):
            c.start()
    x_finish(4, last)
    x_launch(5, last)

    def fold_rest(chunk, v):
        for part in range(3):
            @pl.when(chunk == last)
            def _():
                for c in last_leg(last, part, v):
                    c.wait()
            fold(chunk, v, part)

    def fold_near(i, carry):
        fold_rest(prev + i // 2, 1 + 2 * (i % 2))
        return carry

    lax.fori_loop(0, 4, fold_near, 0)
    for n in (other, node):
        for part in range(3):
            i = pos[ROUTES[part][0]]
            for v, c in enumerate(far_copies(part, n)):
                c.wait()
                accs[part][(i + (1, 3)[v]) % SIDE, n, v * half:(v + 1) * half] += fars[part][v, n]
        for piece in range(2):
            for part in range(3):
                for c in near_copies(part, n, piece):
                    c.start()

    def finish_own(i, carry):
        fold_rest(prev + i, 0)
        return carry

    lax.fori_loop(0, 2, finish_own, 0)

    def finish_x(i, carry):
        x_combine(n_chunks - 3 + i)
        return carry

    lax.fori_loop(0, 3, finish_x, 0)

    def total(part, n, piece):
        for c in near_copies(part, n, piece):
            c.wait()
        at = slice(pieces[piece][0], pieces[piece][0] + pieces[piece][1])
        return (accs[part][pos[ROUTES[part][0]], n, :, at] + nears[part][0, n, :, at] + nears[part][1, n, :, at]).astype(bf16)

    def span_of(part, piece):
        return slice(cols[part][0] + pieces[piece][0], cols[part][0] + pieces[piece][0] + pieces[piece][1])

    def home(at, i):
        c = pltpu.make_async_copy(tok.at[:, pl.ds(at.start, at.stop - at.start)], out_ref.at[:, pl.ds(at.start, at.stop - at.start)], o_sem.at[i])
        c.start()
        return c

    for piece in range(2):
        for part in range(3):
            p_buf[other, :, span_of(part, piece)] = total(part, other, piece)
    p_buf[other, :, rest:] = x_acc[other].astype(bf16)
    share = to_pair(p_buf.at[other], p_recv, 4)
    share.start()
    x_sum = lax.dot_general(pick[node, :cap], x_acc[node].astype(bf16), TN, preferred_element_type=f32)
    share.wait()
    x_sum = x_sum + lax.dot_general(pick[other, :cap], p_recv[:, rest:], TN, preferred_element_type=f32)
    tok[:, rest:] = x_sum.astype(bf16)
    homes = [home(slice(rest, d_model), 0)]
    for part in range(3):
        at = slice(cols[part][0], cols[part][0] + cols[part][1])
        tok[:, at] = lax.dot_general(pick[other, :cap], p_recv[:, at], TN, preferred_element_type=f32).astype(bf16)
    for piece in range(2):
        for part in range(3):
            at = span_of(part, piece)
            mine = lax.dot_general(pick[node, :cap], total(part, node, piece), TN, preferred_element_type=f32)
            tok[:, at] = (tok[:, at].astype(f32) + mine).astype(bf16)
            homes.append(home(at, 1 + piece * 3 + part))
    for c in homes:
        c.wait()


def solution(mesh):
    n_nodes = mesh.shape['node']
    n_ep = mesh.shape['ep']
    row_spec = P(('dp', 'node', 'ep'), None)
    exp_spec = P(('node', 'ep'), None, None)

    def local_layer(tokens, expert_ids, route_w, node_slot, exp_slot, w_gate, w_up, w_down):
        tok_dev, d_model = tokens.shape
        top_k = expert_ids.shape[1]
        d_ff = w_gate.shape[2]
        n_exp = w_gate.shape[0] * n_ep * n_nodes
        limit = max(1, min(top_k, n_nodes // 2))
        cap_node = min(tok_dev, 8 * ((5 * tok_dev * limit + 32 * n_nodes - 1) // (32 * n_nodes)))
        cap_exp = 8 * ((5 * n_nodes * tok_dev * top_k + 32 * n_exp - 1) // (32 * n_exp))
        n_chunks = cap_exp // BLK
        rows = n_ep * BLK

        cube = (SIDE, SIDE, SIDE, BLK, d_model)
        wide = d_model - 3 * part_columns(d_model)[0][1]
        x_cube = (SIDE, SIDE, SIDE, BLK, wide)
        bf16, f32, i32 = jnp.bfloat16, jnp.float32, jnp.int32
        any_spec = pl.BlockSpec(memory_space=pl.ANY)
        dma = pltpu.SemaphoreType.DMA
        out, _, _ = pl.pallas_call(
            functools.partial(moe_kernel, n_chunks),
            name="moe_layer",
            out_shape=(jax.ShapeDtypeStruct((tok_dev, d_model), bf16),
                       jax.ShapeDtypeStruct((n_chunks,) + cube, bf16),
                       jax.ShapeDtypeStruct((n_chunks,) + cube, bf16)),
            in_specs=[any_spec] * 8,
            out_specs=(any_spec, any_spec, any_spec),
            scratch_shapes=[
                pltpu.VMEM((top_k, tok_dev), i32), pltpu.VMEM((top_k, tok_dev), f32),
                pltpu.VMEM((top_k, tok_dev), i32), pltpu.VMEM((top_k, tok_dev), i32),
                pltpu.VMEM((tok_dev, d_model), bf16),
                pltpu.VMEM((2, tok_dev, tok_dev), bf16),
                *[pltpu.VMEM((SIDE, 2, cap_node, width), bf16) for _, width in part_columns(d_model)],
                pltpu.VMEM((2, 2 * top_k, tok_dev), f32), pltpu.VMEM((3, SIDE, 2, 2 * top_k, tok_dev), f32), pltpu.VMEM((2 * top_k, tok_dev), f32),
                pltpu.VMEM((2, cap_node, d_model), bf16), pltpu.VMEM((cap_node, d_model), bf16),
                pltpu.VMEM((2, cap_node, wide), bf16), pltpu.VMEM((2,) + x_cube, bf16), pltpu.VMEM((n_chunks,) + x_cube, bf16),
                pltpu.VMEM((n_chunks,) + x_cube, bf16), pltpu.VMEM((2, cap_node, wide), f32),
                pltpu.VMEM((d_model, d_ff), bf16), pltpu.VMEM((d_model, d_ff), bf16), pltpu.VMEM((d_ff, d_model), bf16),
                pltpu.VMEM((2,) + cube, bf16), pltpu.VMEM((n_chunks,) + cube, bf16), pltpu.VMEM((n_chunks,) + cube, bf16),
                pltpu.VMEM((rows, d_ff), bf16),
                *[pltpu.VMEM((SIDE, 2, cap_node, width), f32) for _, width in part_columns(d_model)],
                *[pltpu.VMEM((2, 2, cap_node // 2, width), f32) for _, width in part_columns(d_model)],
                *[pltpu.VMEM((2, 2, cap_node, width), f32) for _, width in part_columns(d_model)],
                dma((5,)), dma((3,)), dma((4, 2, 3)), dma((4, 2, 3, 3)), dma((4, n_chunks, 3, 3)), dma((9,)), dma((9,)),
                dma((3, 2, 2)), dma((3, 2, 2)), dma((3, 2, 2)), dma((3, 2, 2)), dma((3, 3)), dma((3, 3)),
                dma((3, 2, 2)), dma((3, 2, 2)), dma((3, 2, 2, 2)), dma((3, 2, 2, 2)),
                dma((6, n_chunks, 3)), dma((6, n_chunks, 3)), dma((6, n_chunks)),
                dma((4, 3, 3)), dma((4, 3, 3)), dma((4, 3)), dma((7,)),
            ],
            compiler_params=pltpu.CompilerParams(collective_id=0, has_side_effects=True, vmem_limit_bytes=67_043_328),
        )(expert_ids.T, route_w.T, node_slot.T, exp_slot.T, tokens, w_gate[0], w_up[0], w_down[0])
        return out

    return jax.shard_map(local_layer, mesh=mesh, in_specs=(row_spec,) * 5 + (exp_spec,) * 3, out_specs=row_spec, check_vma=False)
```

```python
import functools

import jax
import jax.numpy as jnp
from jax import lax
from jax.experimental import pallas as pl
from jax.experimental.pallas import tpu as pltpu
from jax.sharding import PartitionSpec as P

MESH = pl.DeviceIdType.MESH
SIDE = 4
SHIFTS = (1, 3, 2)
ROUTES = ((2, 1, 0), (1, 0, 2), (0, 2, 1))
STRIDE = (16, 4, 1)
BLK = 8
SLOTS = 64
NT = (((1,), (1,)), ((), ()))
TN = (((0,), (0,)), ((), ()))


def part_columns(d_model):
    width = d_model // 128 // 3 * 128
    return [(k * width, width) for k in range(3)]


def moe_kernel(n_chunks, ids_hbm, rw_hbm, ns_hbm, es_hbm, tok_hbm, wg_hbm, wu_hbm, wd_hbm, out_ref, mid_d, hop,
               ids, rw, ns, es, tok, pick, rg0, rg1, rg2, own_codes, codes, c_send, p_buf, p_recv, x_rows, x_send, x_leg, x_back, x_acc,
               wg, wu, wd, send1, work, mid_r, hid, acc0, acc1, acc2, far0, far1, far2, near0, near1, near2,
               in_sem, w_sem, own_sem, send_sem, recv_sem, pair_send, pair_recv, a_send, a_recv, b_send, b_recv, c_ssem, c_rsem,
               f_send, f_recv, n_send, n_recv, x_ssem, x_rsem, x_osem, l_send, l_recv, l_own, o_sem):
    f32, bf16 = jnp.float32, jnp.bfloat16
    tok_dev, d_model = tok_hbm.shape
    d_ff = wg_hbm.shape[1]
    top_k = ids_hbm.shape[0]
    n_ep = SIDE ** 3
    rows = n_ep * BLK
    cap = p_recv.shape[0]
    half = cap // 2
    node = lax.axis_index("node")
    other = 1 - node
    ep = lax.axis_index("ep")
    pos = (ep // (SIDE * SIDE), (ep // SIDE) % SIDE, ep % SIDE)
    cols = part_columns(d_model)
    rest = cols[2][0] + cols[2][1]
    rings, accs, fars, nears = (rg0, rg1, rg2), (acc0, acc1, acc2), (far0, far1, far2), (near0, near1, near2)

    def peer(dim, shift):
        at = [pos[0], pos[1], pos[2]]
        at[dim] = (pos[dim] + shift) % SIDE
        return (at[0] * SIDE + at[1]) * SIDE + at[2]

    def to_ep(src, dst, ssem, rsem, dim, shift):
        return pltpu.make_async_remote_copy(src_ref=src, dst_ref=dst, send_sem=ssem, recv_sem=rsem,
                                            device_id={"ep": peer(dim, shift)}, device_id_type=MESH)

    def to_pair(src, dst, i):
        return pltpu.make_async_remote_copy(src_ref=src, dst_ref=dst, send_sem=pair_send.at[i], recv_sem=pair_recv.at[i],
                                            device_id={"node": other}, device_id_type=MESH)

    def drain(ref, *sems):
        for sem in sems:
            pltpu.make_async_copy(ref, ref, sem).wait()

    inputs = [pltpu.make_async_copy(s, d, in_sem.at[i]) for i, (s, d) in enumerate(
        ((ids_hbm, ids), (rw_hbm, rw), (ns_hbm, ns), (es_hbm, es), (tok_hbm, tok)))]
    weights = [pltpu.make_async_copy(s, d, w_sem.at[i]) for i, (s, d) in enumerate(((wg_hbm, wg), (wu_hbm, wu), (wd_hbm, wd)))]
    for c in inputs:
        c.start()
    barrier = pltpu.get_barrier_semaphore()
    pl.semaphore_signal(barrier, inc=1, device_id={"node": other}, device_id_type=MESH)
    for dim in range(3):
        for shift in SHIFTS:
            pl.semaphore_signal(barrier, inc=1, device_id={"ep": peer(dim, shift)}, device_id_type=MESH)
    for c in inputs:
        c.wait()

    def on_group(m):
        return (ids[...] >= m * n_ep) & (ids[...] < (m + 1) * n_ep)

    def find_rows(m):
        slot = jnp.max(jnp.where(on_group(m), ns[...], -1), axis=0, keepdims=True)
        pick[m] = jnp.where(lax.broadcasted_iota(jnp.int32, (tok_dev, tok_dev), 0) == slot, 1.0, 0.0).astype(bf16)

    def route(m):
        kept = on_group(m) & (ns[...] >= 0) & (es[...] >= 0)
        a = jnp.where(kept, (ids[...] - m * n_ep) * SLOTS, 0).astype(f32)
        b = jnp.where(kept, es[...] + 1, 0).astype(f32)
        w = jnp.where(kept, rw[...], 0.0)
        w1 = w.astype(bf16).astype(f32)
        w2 = (w - w1).astype(bf16).astype(f32)
        w3 = w - w1 - w2
        parts = [jnp.concatenate([p, q], axis=0).astype(bf16) for p, q in ((a, w1), (b, w2), (jnp.zeros_like(a), w3))]
        return sum(lax.dot_general(p, pick[m], NT, preferred_element_type=f32) for p in parts[::-1])

    find_rows(node)
    for part in range(3):
        c0, width = cols[part]
        rings[part][pos[ROUTES[part][0]], node] = jnp.dot(
            pick[node, :cap], tok[:, c0:c0 + width], preferred_element_type=f32).astype(bf16)
    x_rows[node] = jnp.dot(pick[node, :cap], tok[:, rest:], preferred_element_type=f32).astype(bf16)
    pl.semaphore_wait(barrier, 1 + 3 * len(SHIFTS))

    def ring_copies(part, n):
        dim, ring = ROUTES[part][0], rings[part]
        i = pos[dim]
        first = [to_ep(ring.at[i, n], ring.at[i, n], a_send.at[part, n], a_recv.at[part, n], dim, (1, 3)[v]) for v in range(2)]
        onward = []
        for v in range(2):
            k = (i + (3, 1)[v]) % SIDE
            span = pl.ds(v * half, half)
            onward.append(to_ep(ring.at[k, n, span], ring.at[k, n, span], b_send.at[part, n], b_recv.at[part, n], dim, (1, 3)[v]))
        return first, onward

    for part in range(3):
        for c in ring_copies(part, node)[0]:
            c.start()
    find_rows(other)
    p_buf[other] = jnp.dot(pick[other, :cap], tok[...], preferred_element_type=f32).astype(bf16)
    pair = [to_pair(p_buf.at[other, :, pl.ds(*cols[part])], rings[part].at[pos[ROUTES[part][0]], node], part) for part in range(3)]
    pair.append(to_pair(p_buf.at[other, :, pl.ds(rest, d_model - rest)], x_rows.at[node], 7))
    for c in pair:
        c.start()
    c_send[...] = route(other)
    pair_codes = to_pair(c_send, own_codes.at[node], 3)
    pair_codes.start()
    own_codes[node] = route(node)
    for c in weights:
        c.start()
    for acc in accs:
        acc[...] = jnp.zeros_like(acc)
    for c in pair:
        c.wait()
    for part in range(3):
        for c in ring_copies(part, other)[0]:
            c.start()
    pair_codes.wait()
    code_copies = [to_ep(own_codes, codes.at[dim, pos[dim]], c_ssem.at[dim], c_rsem.at[dim], dim, shift)
                   for dim in range(3) for shift in SHIFTS]
    for c in code_copies:
        c.start()
    for dim in range(3):
        codes[dim, pos[dim]] = own_codes[...]
    stages = ((send1, mid_d, 1), (mid_d, work, 2), (work, hop, 2), (hop, mid_r, 1))

    def plane(ref, chunk, dim, index, part):
        c0, width = cols[part]
        idx = [chunk, slice(None), slice(None), slice(None), slice(None), pl.ds(c0, width)]
        idx[1 + dim] = index
        return ref.at[tuple(idx)]

    def copies(stage, chunk):
        src, dst, leg = stages[stage]
        src_chunk = chunk % 2 if stage == 0 else chunk
        remote, local = [], []
        for part in range(3):
            dim = ROUTES[part][leg]
            for v, shift in enumerate(SHIFTS):
                remote.append(to_ep(plane(src, src_chunk, dim, (pos[dim] + shift) % SIDE, part),
                                    plane(dst, chunk, dim, pos[dim], part),
                                    send_sem.at[stage, chunk % 2], recv_sem.at[stage, chunk], dim, shift))
            local.append(pltpu.make_async_copy(
                plane(src, src_chunk, dim, pos[dim], part), plane(dst, chunk, dim, pos[dim], part),
                own_sem.at[stage, chunk % 2]))
        return remote, local

    def launch(stage, chunk):
        remote, local = copies(stage, chunk)
        for c in remote:
            c.start()
        for c in local:
            c.start()

    def all_of(ref, chunk, planes):
        return ref.at[chunk, pl.ds(0, planes), :, :, :, pl.ds(0, rest)]

    def finish(stage, chunk):
        dst = stages[stage][1]
        drain(all_of(dst, chunk, 3), send_sem.at[stage, chunk % 2], recv_sem.at[stage, chunk])
        drain(all_of(dst, chunk, 1), own_sem.at[stage, chunk % 2])

    def plane_codes(chunk, dim, at):
        o0, o1 = [d for d in range(3) if d != dim]
        r = lax.broadcasted_iota(jnp.int32, (SIDE * SIDE * BLK, cap), 0)
        expert = at * STRIDE[dim] + (r >> 5) * STRIDE[o0] + ((r >> 3) & 3) * STRIDE[o1]
        return (expert * SLOTS + (r & 7) + chunk * BLK + 1).astype(f32)

    def pick_slots(want, code, packed):
        block = None
        for n in range(2):
            hit = jnp.zeros(want.shape, f32)
            for j in range(top_k):
                hit = jnp.where(code[n, j:j + 1, :cap] == want, 1.0, hit)
            got = jnp.dot(hit.astype(bf16), packed[n], preferred_element_type=f32)
            block = got if block is None else block + got
        return block.astype(bf16).reshape(SIDE, SIDE, BLK, -1)

    def weigh_slots(want, code, y, n):
        w = jnp.zeros(want.shape, f32)
        for j in range(top_k):
            w = jnp.where(code[n, j:j + 1, :cap] == want, code[n, top_k + j:top_k + j + 1, :cap], w)
        hi = w.astype(bf16)
        left = w - hi.astype(f32)
        mid = left.astype(bf16)
        lo = (left - mid.astype(f32)).astype(bf16)
        return lax.dot_general(jnp.concatenate([lo, mid, hi], axis=0), jnp.concatenate([y, y, y], axis=0), TN, preferred_element_type=f32)

    x_stages = ((x_send, x_leg), (x_leg, mid_d), (mid_d, work), (work, hop), (hop, mid_r), (mid_r, x_back))

    def x_copies(leg, chunk, route_no):
        src, dst = x_stages[leg]
        dim = ROUTES[route_no][leg if leg < 3 else 5 - leg]

        def at(ref, index):
            c0 = 0 if ref.shape[-1] == d_model - rest else rest
            idx = [chunk % 2 if ref is x_send else chunk, slice(None), slice(None), slice(None), slice(None), pl.ds(c0, d_model - rest)]
            idx[1 + dim] = index
            return ref.at[tuple(idx)]

        remote = [to_ep(at(src, (pos[dim] + shift) % SIDE), at(dst, pos[dim]), x_ssem.at[leg, chunk], x_rsem.at[leg, chunk], dim, shift)
                  for shift in SHIFTS]
        return remote + [pltpu.make_async_copy(at(src, pos[dim]), at(dst, pos[dim]), x_osem.at[leg, chunk])]

    def x_launch(leg, chunk):
        for route_no in range(3):
            @pl.when(chunk % 3 == route_no)
            def _():
                for c in x_copies(leg, chunk, route_no):
                    c.start()

    def x_finish(leg, chunk):
        drain(x_leg.at[chunk, pl.ds(0, 3)], x_ssem.at[leg, chunk], x_rsem.at[leg, chunk])
        drain(x_leg.at[chunk, 0], x_osem.at[leg, chunk])

    def x_gather(chunk):
        def pick_plane(z, carry):
            x_send[chunk % 2, z] = pick_slots(plane_codes(chunk, 0, z), own_codes, x_rows)
            return carry

        lax.fori_loop(0, SIDE, pick_plane, 0)
        x_launch(0, chunk)

    def x_combine(chunk):
        x_finish(5, chunk)

        def add_plane(z, carry):
            y = x_back[chunk, z].reshape(SIDE * SIDE * BLK, d_model - rest)
            want = plane_codes(chunk, 0, z)
            for n in range(2):
                x_acc[n] += weigh_slots(want, own_codes, y, n)
            return carry

        lax.fori_loop(0, SIDE, add_plane, 0)

    x_acc[...] = jnp.zeros_like(x_acc)
    x_gather(0)
    for n in (node, other):
        for part in range(3):
            drain(rings[part].at[pl.ds(0, 2), n], a_send.at[part, n], a_recv.at[part, n])
            for c in ring_copies(part, n)[1]:
                c.start()
    for dim in range(3):
        drain(codes.at[dim, pl.ds(0, 3)], c_ssem.at[dim], c_rsem.at[dim])

    def line(ref, slot, part, k, index):
        idx = [slot, slice(None), slice(None), slice(None), slice(None), pl.ds(*cols[part])]
        idx[1 + ROUTES[part][0]], idx[1 + ROUTES[part][1]] = k, index
        return ref.at[tuple(idx)]

    def first_leg(chunk, part, k):
        dim = ROUTES[part][1]
        for v, shift in enumerate(SHIFTS):
            to_ep(line(send1, chunk % 2, part, k, (pos[dim] + shift) % SIDE), line(mid_d, chunk, part, k, pos[dim]),
                  send_sem.at[0, chunk % 2], recv_sem.at[0, chunk], dim, shift).start()
        pltpu.make_async_copy(line(send1, chunk % 2, part, k, pos[dim]), line(mid_d, chunk, part, k, pos[dim]),
                              own_sem.at[0, chunk % 2]).start()

    def last_leg(chunk, part, v):
        dim = ROUTES[part][1]
        k = (pos[ROUTES[part][0]] + v) % SIDE
        made = [to_ep(line(hop, chunk, part, k, (pos[dim] + shift) % SIDE), line(mid_r, chunk, part, k, pos[dim]),
                      l_send.at[v], l_recv.at[v], dim, shift) for shift in SHIFTS]
        return made + [pltpu.make_async_copy(line(hop, chunk, part, k, pos[dim]), line(mid_r, chunk, part, k, pos[dim]), l_own.at[v])]

    def last_finish(chunk, v):
        drain(mid_r.at[chunk, 0, pl.ds(0, 3), :, :, pl.ds(0, rest)], l_send.at[v], l_recv.at[v])
        drain(mid_r.at[chunk, 0, 0, :, :, pl.ds(0, rest)], l_own.at[v])

    def gather(chunk):
        for v in (0, 3, 1, 2):
            for part in range(3):
                if v == 2:
                    @pl.when(chunk == 0)
                    def _():
                        for n in (node, other):
                            drain(rings[part].at[0, n], b_send.at[part, n], b_recv.at[part, n])
                dim = ROUTES[part][0]
                k = (pos[dim] + v) % SIDE
                c0, width = cols[part]
                idx = [chunk % 2, slice(None), slice(None), slice(None), slice(None), slice(c0, c0 + width)]
                idx[1 + dim] = k
                send1[tuple(idx)] = pick_slots(plane_codes(chunk, dim, pos[dim]), codes.at[dim, k], rings[part].at[k])
                first_leg(chunk, part, k)

    def ffn(chunk):
        width = 256

        def up(n, carry):
            at = pl.ds(pl.multiple_of(n * width, width), width)
            x = work[chunk].reshape(rows, d_model)
            g = jnp.dot(x, wg[:, at], preferred_element_type=f32)
            u = jnp.dot(x, wu[:, at], preferred_element_type=f32)
            hid[:, at] = (jax.nn.silu(g) * u).astype(bf16)
            return carry

        lax.fori_loop(0, d_ff // width, up, 0)

        def down(n, carry):
            at = pl.ds(pl.multiple_of(n * width, width), width)
            y = jnp.dot(hid[...], wd[:, at], preferred_element_type=f32)
            work[chunk, :, :, :, :, at] = y.reshape(SIDE, SIDE, SIDE, BLK, width).astype(bf16)
            return carry

        lax.fori_loop(0, d_model // width, down, 0)

    def fold(chunk, v, part):
        dim = ROUTES[part][0]
        k = (pos[dim] + v) % SIDE
        c0, width = cols[part]
        want = plane_codes(chunk, dim, pos[dim])
        idx = [chunk, slice(None), slice(None), slice(None), slice(None), slice(c0, c0 + width)]
        idx[1 + dim] = k
        y = mid_r[tuple(idx)].reshape(SIDE * SIDE * BLK, width)
        for n in range(2):
            accs[part][k, n] += weigh_slots(want, codes.at[dim, k], y, n)

    def step(t, carry):
        @pl.when(t < n_chunks)
        def _():
            gather(t)
            x_finish(0, t)
            x_launch(1, t)

        @pl.when(t + 1 < n_chunks)
        def _():
            x_gather(t + 1)

        for stage in range(1, 5):
            chunk = t - stage

            @pl.when((chunk >= 0) & (chunk < (n_chunks if stage < 4 else n_chunks - 1)))
            def _():
                finish(stage - 1, chunk)
                x_finish(stage, chunk)
                if stage == 2:
                    @pl.when(chunk == 0)
                    def _():
                        for c in weights:
                            c.wait()
                    ffn(chunk)
                x_launch(stage + 1, chunk)
                if stage < 4:
                    launch(stage, chunk)
                else:
                    def fold_source(v, carry):
                        for part in range(3):
                            fold(chunk, v, part)
                        return carry

                    lax.fori_loop(0, SIDE, fold_source, 0)

        @pl.when(t >= 5)
        def _():
            x_combine(t - 5)

        return carry

    lax.fori_loop(0, n_chunks + 2, step, 0)

    def far_copies(part, n):
        dim = ROUTES[part][0]
        k = (pos[dim] + 2) % SIDE
        return [to_ep(accs[part].at[k, n, pl.ds(v * half, half)], fars[part].at[v, n], f_send.at[part, n], f_recv.at[part, n],
                      dim, (1, 3)[v]) for v in range(2)]

    first = (cols[0][1] // 128 + 1) // 2 * 128
    pieces = ((0, first), (first, cols[0][1] - first))

    def near_copies(part, n, piece):
        dim = ROUTES[part][0]
        span = pl.ds(*pieces[piece])
        return [to_ep(accs[part].at[(pos[dim] + (1, 3)[v]) % SIDE, n, :, span], nears[part].at[v, n, :, span],
                      n_send.at[part, n, piece], n_recv.at[part, n, piece], dim, (1, 3)[v]) for v in range(2)]

    last, prev = n_chunks - 1, n_chunks - 2

    finish(2, last)
    x_finish(3, last)

    def start_source(i, carry):
        for part in range(3):
            for c in last_leg(last, part, (2 + 3 * i) % SIDE):
                c.start()
        return carry

    lax.fori_loop(0, SIDE, start_source, 0)
    x_launch(4, last)
    finish(3, prev)
    x_finish(4, prev)
    x_launch(5, prev)

    def fold_far(i, carry):
        @pl.when(i == 1)
        def _():
            last_finish(last, 2)

        for part in range(3):
            fold(prev + i, 2, part)

            @pl.when(i == 1)
            def _():
                for c in far_copies(part, other):
                    c.start()
        return carry

    lax.fori_loop(0, 2, fold_far, 0)
    for part in range(3):
        for c in far_copies(part, node):
            c.start()
    x_finish(4, last)
    x_launch(5, last)

    def fold_rest(chunk, v):
        @pl.when(chunk == last)
        def _():
            last_finish(last, v)

        for part in range(3):
            fold(chunk, v, part)

    def fold_near(i, carry):
        fold_rest(prev + i // 2, 1 + 2 * (i % 2))
        return carry

    lax.fori_loop(0, 4, fold_near, 0)
    for n in (other, node):
        for part in range(3):
            i = pos[ROUTES[part][0]]
            drain(fars[part].at[:, n], f_send.at[part, n], f_recv.at[part, n])
            for v in range(2):
                accs[part][(i + (1, 3)[v]) % SIDE, n, v * half:(v + 1) * half] += fars[part][v, n]
        for piece in range(2):
            for part in range(3):
                for c in near_copies(part, n, piece):
                    c.start()

    def finish_own(i, carry):
        fold_rest(prev + i, 0)
        return carry

    lax.fori_loop(0, 2, finish_own, 0)

    def finish_x(i, carry):
        x_combine(n_chunks - 3 + i)
        return carry

    lax.fori_loop(0, 3, finish_x, 0)

    def total(part, n, piece):
        drain(nears[part].at[:, n, :, pl.ds(*pieces[piece])], n_send.at[part, n, piece], n_recv.at[part, n, piece])
        at = slice(pieces[piece][0], pieces[piece][0] + pieces[piece][1])
        return (accs[part][pos[ROUTES[part][0]], n, :, at] + nears[part][0, n, :, at] + nears[part][1, n, :, at]).astype(bf16)

    def span_of(part, piece):
        return slice(cols[part][0] + pieces[piece][0], cols[part][0] + pieces[piece][0] + pieces[piece][1])

    def home(at, i):
        c = pltpu.make_async_copy(tok.at[:, pl.ds(at.start, at.stop - at.start)], out_ref.at[:, pl.ds(at.start, at.stop - at.start)], o_sem.at[i])
        c.start()
        return c

    for piece in range(2):
        for part in range(3):
            p_buf[other, :, span_of(part, piece)] = total(part, other, piece)
    p_buf[other, :, rest:] = x_acc[other].astype(bf16)
    share = to_pair(p_buf.at[other], p_recv, 4)
    share.start()
    x_sum = lax.dot_general(pick[node, :cap], x_acc[node].astype(bf16), TN, preferred_element_type=f32)
    share.wait()
    x_sum = x_sum + lax.dot_general(pick[other, :cap], p_recv[:, rest:], TN, preferred_element_type=f32)
    tok[:, rest:] = x_sum.astype(bf16)
    homes = [home(slice(rest, d_model), 0)]
    for part in range(3):
        at = slice(cols[part][0], cols[part][0] + cols[part][1])
        tok[:, at] = lax.dot_general(pick[other, :cap], p_recv[:, at], TN, preferred_element_type=f32).astype(bf16)
    for piece in range(2):
        for part in range(3):
            at = span_of(part, piece)
            mine = lax.dot_general(pick[node, :cap], total(part, node, piece), TN, preferred_element_type=f32)
            tok[:, at] = (tok[:, at].astype(f32) + mine).astype(bf16)
            homes.append(home(at, 1 + piece * 3 + part))
    for c in homes:
        c.wait()


def solution(mesh):
    n_nodes = mesh.shape['node']
    n_ep = mesh.shape['ep']
    row_spec = P(('dp', 'node', 'ep'), None)
    exp_spec = P(('node', 'ep'), None, None)

    def local_layer(tokens, expert_ids, route_w, node_slot, exp_slot, w_gate, w_up, w_down):
        tok_dev, d_model = tokens.shape
        top_k = expert_ids.shape[1]
        d_ff = w_gate.shape[2]
        n_exp = w_gate.shape[0] * n_ep * n_nodes
        limit = max(1, min(top_k, n_nodes // 2))
        cap_node = min(tok_dev, 8 * ((5 * tok_dev * limit + 32 * n_nodes - 1) // (32 * n_nodes)))
        cap_exp = 8 * ((5 * n_nodes * tok_dev * top_k + 32 * n_exp - 1) // (32 * n_exp))
        n_chunks = cap_exp // BLK
        rows = n_ep * BLK

        cube = (SIDE, SIDE, SIDE, BLK, d_model)
        wide = d_model - 3 * part_columns(d_model)[0][1]
        x_cube = (SIDE, SIDE, SIDE, BLK, wide)
        bf16, f32, i32 = jnp.bfloat16, jnp.float32, jnp.int32
        any_spec = pl.BlockSpec(memory_space=pl.ANY)
        dma = pltpu.SemaphoreType.DMA
        out, _, _ = pl.pallas_call(
            functools.partial(moe_kernel, n_chunks),
            name="moe_layer",
            out_shape=(jax.ShapeDtypeStruct((tok_dev, d_model), bf16),
                       jax.ShapeDtypeStruct((n_chunks,) + cube, bf16),
                       jax.ShapeDtypeStruct((n_chunks,) + cube, bf16)),
            in_specs=[any_spec] * 8,
            out_specs=(any_spec, any_spec, any_spec),
            scratch_shapes=[
                pltpu.VMEM((top_k, tok_dev), i32), pltpu.VMEM((top_k, tok_dev), f32),
                pltpu.VMEM((top_k, tok_dev), i32), pltpu.VMEM((top_k, tok_dev), i32),
                pltpu.VMEM((tok_dev, d_model), bf16),
                pltpu.VMEM((2, tok_dev, tok_dev), bf16),
                *[pltpu.VMEM((SIDE, 2, cap_node, width), bf16) for _, width in part_columns(d_model)],
                pltpu.VMEM((2, 2 * top_k, tok_dev), f32), pltpu.VMEM((3, SIDE, 2, 2 * top_k, tok_dev), f32), pltpu.VMEM((2 * top_k, tok_dev), f32),
                pltpu.VMEM((2, cap_node, d_model), bf16), pltpu.VMEM((cap_node, d_model), bf16),
                pltpu.VMEM((2, cap_node, wide), bf16), pltpu.VMEM((2,) + x_cube, bf16), pltpu.VMEM((n_chunks,) + x_cube, bf16),
                pltpu.VMEM((n_chunks,) + x_cube, bf16), pltpu.VMEM((2, cap_node, wide), f32),
                pltpu.VMEM((d_model, d_ff), bf16), pltpu.VMEM((d_model, d_ff), bf16), pltpu.VMEM((d_ff, d_model), bf16),
                pltpu.VMEM((2,) + cube, bf16), pltpu.VMEM((n_chunks,) + cube, bf16), pltpu.VMEM((n_chunks,) + cube, bf16),
                pltpu.VMEM((rows, d_ff), bf16),
                *[pltpu.VMEM((SIDE, 2, cap_node, width), f32) for _, width in part_columns(d_model)],
                *[pltpu.VMEM((2, 2, cap_node // 2, width), f32) for _, width in part_columns(d_model)],
                *[pltpu.VMEM((2, 2, cap_node, width), f32) for _, width in part_columns(d_model)],
                dma((5,)), dma((3,)), dma((4, 2)), dma((4, 2)), dma((4, n_chunks)), dma((9,)), dma((9,)),
                dma((3, 2)), dma((3, 2)), dma((3, 2)), dma((3, 2)), dma((3,)), dma((3,)),
                dma((3, 2)), dma((3, 2)), dma((3, 2, 2)), dma((3, 2, 2)),
                dma((6, n_chunks)), dma((6, n_chunks)), dma((6, n_chunks)),
                dma((4,)), dma((4,)), dma((4,)), dma((7,)),
            ],
            compiler_params=pltpu.CompilerParams(collective_id=0, has_side_effects=True, vmem_limit_bytes=67_043_328),
        )(expert_ids.T, route_w.T, node_slot.T, exp_slot.T, tokens, w_gate[0], w_up[0], w_down[0])
        return out

    return jax.shard_map(local_layer, mesh=mesh, in_specs=(row_spec,) * 5 + (exp_spec,) * 3, out_specs=row_spec, check_vma=False)
```

```python
import functools

import jax
import jax.numpy as jnp
from jax import lax
from jax.experimental import pallas as pl
from jax.experimental.pallas import tpu as pltpu
from jax.sharding import PartitionSpec as P

MESH = pl.DeviceIdType.MESH
SIDE = 4
SHIFTS = (1, 3, 2)
ROUTES = ((2, 1, 0), (1, 0, 2), (0, 2, 1))
STRIDE = (16, 4, 1)
BLK = 8
SLOTS = 64
NT = (((1,), (1,)), ((), ()))
TN = (((0,), (0,)), ((), ()))


def part_columns(d_model):
    width = d_model // 128 // 3 * 128
    return [(k * width, width) for k in range(3)]


def moe_kernel(n_chunks, ids_hbm, rw_hbm, ns_hbm, es_hbm, tok_hbm, wg_hbm, wu_hbm, wd_hbm, out_ref, mid_d, hop,
               ids, rw, ns, es, tok, pick, rg0, rg1, rg2, own_codes, codes, c_send, p_buf, p_recv, x_rows, x_send, x_leg, x_back, x_acc,
               wg, wu, wd, send1, work, mid_r, hid, acc0, acc1, acc2, far0, far1, far2, near0, near1, near2,
               in_sem, w_sem, own_sem, send_sem, recv_sem, pair_send, pair_recv, a_send, a_recv, b_send, b_recv, c_ssem, c_rsem,
               f_send, f_recv, n_send, n_recv, x_ssem, x_rsem, x_osem, l_send, l_recv, l_own, o_sem):
    f32, bf16 = jnp.float32, jnp.bfloat16
    tok_dev, d_model = tok_hbm.shape
    d_ff = wg_hbm.shape[1]
    top_k = ids_hbm.shape[0]
    n_ep = SIDE ** 3
    rows = n_ep * BLK
    cap = p_recv.shape[0]
    half = cap // 2
    node = lax.axis_index("node")
    other = 1 - node
    ep = lax.axis_index("ep")
    pos = (ep // (SIDE * SIDE), (ep // SIDE) % SIDE, ep % SIDE)
    cols = part_columns(d_model)
    rest = cols[2][0] + cols[2][1]
    rings, accs, fars, nears = (rg0, rg1, rg2), (acc0, acc1, acc2), (far0, far1, far2), (near0, near1, near2)

    def peer(dim, shift):
        at = [pos[0], pos[1], pos[2]]
        at[dim] = (pos[dim] + shift) % SIDE
        return (at[0] * SIDE + at[1]) * SIDE + at[2]

    def to_ep(src, dst, ssem, rsem, dim, shift):
        return pltpu.make_async_remote_copy(src_ref=src, dst_ref=dst, send_sem=ssem, recv_sem=rsem,
                                            device_id={"ep": peer(dim, shift)}, device_id_type=MESH)

    def to_pair(src, dst, i):
        return pltpu.make_async_remote_copy(src_ref=src, dst_ref=dst, send_sem=pair_send.at[i], recv_sem=pair_recv.at[i],
                                            device_id={"node": other}, device_id_type=MESH)

    def drain(ref, *sems):
        for sem in sems:
            pltpu.make_async_copy(ref, ref, sem).wait()

    inputs = [pltpu.make_async_copy(s, d, in_sem.at[i]) for i, (s, d) in enumerate(
        ((ids_hbm, ids), (rw_hbm, rw), (ns_hbm, ns), (es_hbm, es), (tok_hbm, tok)))]
    weights = [pltpu.make_async_copy(s, d, w_sem.at[i]) for i, (s, d) in enumerate(((wg_hbm, wg), (wu_hbm, wu), (wd_hbm, wd)))]
    for c in inputs:
        c.start()
    barrier = pltpu.get_barrier_semaphore()
    pl.semaphore_signal(barrier, inc=1, device_id={"node": other}, device_id_type=MESH)
    for dim in range(3):
        for shift in SHIFTS:
            pl.semaphore_signal(barrier, inc=1, device_id={"ep": peer(dim, shift)}, device_id_type=MESH)
    for c in inputs:
        c.wait()

    def on_group(m):
        return (ids[...] >= m * n_ep) & (ids[...] < (m + 1) * n_ep)

    def find_rows(m):
        slot = jnp.max(jnp.where(on_group(m), ns[...], -1), axis=0, keepdims=True)
        pick[m] = jnp.where(lax.broadcasted_iota(jnp.int32, (tok_dev, tok_dev), 0) == slot, 1.0, 0.0).astype(bf16)

    def route(m):
        kept = on_group(m) & (ns[...] >= 0) & (es[...] >= 0)
        a = jnp.where(kept, (ids[...] - m * n_ep) * SLOTS, 0).astype(f32)
        b = jnp.where(kept, es[...] + 1, 0).astype(f32)
        w = jnp.where(kept, rw[...], 0.0)
        w1 = w.astype(bf16).astype(f32)
        w2 = (w - w1).astype(bf16).astype(f32)
        w3 = w - w1 - w2
        parts = [jnp.concatenate([p, q], axis=0).astype(bf16) for p, q in ((a, w1), (b, w2), (jnp.zeros_like(a), w3))]
        return sum(lax.dot_general(p, pick[m], NT, preferred_element_type=f32) for p in parts[::-1])

    find_rows(node)
    for part in range(3):
        c0, width = cols[part]
        rings[part][pos[ROUTES[part][0]], node] = jnp.dot(
            pick[node, :cap], tok[:, c0:c0 + width], preferred_element_type=f32).astype(bf16)
    x_rows[node] = jnp.dot(pick[node, :cap], tok[:, rest:], preferred_element_type=f32).astype(bf16)
    pl.semaphore_wait(barrier, 1 + 3 * len(SHIFTS))

    def ring_copies(part, n):
        dim, ring = ROUTES[part][0], rings[part]
        i = pos[dim]
        first = [to_ep(ring.at[i, n], ring.at[i, n], a_send.at[part, n], a_recv.at[part, n], dim, (1, 3)[v]) for v in range(2)]
        onward = []
        for v in range(2):
            k = (i + (3, 1)[v]) % SIDE
            span = pl.ds(v * half, half)
            onward.append(to_ep(ring.at[k, n, span], ring.at[k, n, span], b_send.at[part, n], b_recv.at[part, n], dim, (1, 3)[v]))
        return first, onward

    for part in range(3):
        for c in ring_copies(part, node)[0]:
            c.start()
    find_rows(other)
    p_buf[other] = jnp.dot(pick[other, :cap], tok[...], preferred_element_type=f32).astype(bf16)
    pair = [to_pair(p_buf.at[other, :, pl.ds(*cols[part])], rings[part].at[pos[ROUTES[part][0]], node], 0) for part in range(3)]
    pair.append(to_pair(p_buf.at[other, :, pl.ds(rest, d_model - rest)], x_rows.at[node], 0))
    for c in pair:
        c.start()
    c_send[...] = route(other)
    pair_codes = to_pair(c_send, own_codes.at[node], 3)
    pair_codes.start()
    own_codes[node] = route(node)
    for c in weights:
        c.start()
    for acc in accs:
        acc[...] = jnp.zeros_like(acc)
    drain(p_buf.at[other], pair_send.at[0], pair_recv.at[0])
    for part in range(3):
        for c in ring_copies(part, other)[0]:
            c.start()
    pair_codes.wait()
    code_copies = [to_ep(own_codes, codes.at[dim, pos[dim]], c_ssem.at[dim], c_rsem.at[dim], dim, shift)
                   for dim in range(3) for shift in SHIFTS]
    for c in code_copies:
        c.start()
    for dim in range(3):
        codes[dim, pos[dim]] = own_codes[...]
    stages = ((send1, mid_d, 1), (mid_d, work, 2), (work, hop, 2), (hop, mid_r, 1))

    def plane(ref, chunk, dim, index, part):
        c0, width = cols[part]
        idx = [chunk, slice(None), slice(None), slice(None), slice(None), pl.ds(c0, width)]
        idx[1 + dim] = index
        return ref.at[tuple(idx)]

    def copies(stage, chunk):
        src, dst, leg = stages[stage]
        src_chunk = chunk % 2 if stage == 0 else chunk
        remote, local = [], []
        for part in range(3):
            dim = ROUTES[part][leg]
            for v, shift in enumerate(SHIFTS):
                remote.append(to_ep(plane(src, src_chunk, dim, (pos[dim] + shift) % SIDE, part),
                                    plane(dst, chunk, dim, pos[dim], part),
                                    send_sem.at[stage, chunk % 2], recv_sem.at[stage, chunk], dim, shift))
            local.append(pltpu.make_async_copy(
                plane(src, src_chunk, dim, pos[dim], part), plane(dst, chunk, dim, pos[dim], part),
                own_sem.at[stage, chunk % 2]))
        return remote, local

    def launch(stage, chunk):
        remote, local = copies(stage, chunk)
        for c in remote:
            c.start()
        for c in local:
            c.start()

    def all_of(ref, chunk, planes):
        return ref.at[chunk, pl.ds(0, planes), :, :, :, pl.ds(0, rest)]

    def finish(stage, chunk):
        dst = stages[stage][1]
        drain(all_of(dst, chunk, 3), send_sem.at[stage, chunk % 2], recv_sem.at[stage, chunk])
        drain(all_of(dst, chunk, 1), own_sem.at[stage, chunk % 2])

    def plane_codes(chunk, dim, at):
        o0, o1 = [d for d in range(3) if d != dim]
        r = lax.broadcasted_iota(jnp.int32, (SIDE * SIDE * BLK, cap), 0)
        expert = at * STRIDE[dim] + (r >> 5) * STRIDE[o0] + ((r >> 3) & 3) * STRIDE[o1]
        return (expert * SLOTS + (r & 7) + chunk * BLK + 1).astype(f32)

    def pick_slots(want, code, packed):
        block = None
        for n in range(2):
            hit = jnp.zeros(want.shape, f32)
            for j in range(top_k):
                hit = jnp.where(code[n, j:j + 1, :cap] == want, 1.0, hit)
            got = jnp.dot(hit.astype(bf16), packed[n], preferred_element_type=f32)
            block = got if block is None else block + got
        return block.astype(bf16).reshape(SIDE, SIDE, BLK, -1)

    def weigh_slots(want, code, y, n):
        w = jnp.zeros(want.shape, f32)
        for j in range(top_k):
            w = jnp.where(code[n, j:j + 1, :cap] == want, code[n, top_k + j:top_k + j + 1, :cap], w)
        hi = w.astype(bf16)
        left = w - hi.astype(f32)
        mid = left.astype(bf16)
        lo = (left - mid.astype(f32)).astype(bf16)
        return lax.dot_general(jnp.concatenate([lo, mid, hi], axis=0), jnp.concatenate([y, y, y], axis=0), TN, preferred_element_type=f32)

    x_stages = ((x_send, x_leg), (x_leg, mid_d), (mid_d, work), (work, hop), (hop, mid_r), (mid_r, x_back))

    def x_copies(leg, chunk, route_no):
        src, dst = x_stages[leg]
        dim = ROUTES[route_no][leg if leg < 3 else 5 - leg]

        def at(ref, index):
            c0 = 0 if ref.shape[-1] == d_model - rest else rest
            idx = [chunk % 2 if ref is x_send else chunk, slice(None), slice(None), slice(None), slice(None), pl.ds(c0, d_model - rest)]
            idx[1 + dim] = index
            return ref.at[tuple(idx)]

        remote = [to_ep(at(src, (pos[dim] + shift) % SIDE), at(dst, pos[dim]), x_ssem.at[leg, chunk % 2], x_rsem.at[leg, chunk], dim, shift)
                  for shift in SHIFTS]
        return remote + [pltpu.make_async_copy(at(src, pos[dim]), at(dst, pos[dim]), x_osem.at[leg, chunk % 2])]

    def x_launch(leg, chunk):
        for route_no in range(3):
            @pl.when(chunk % 3 == route_no)
            def _():
                for c in x_copies(leg, chunk, route_no):
                    c.start()

    def x_finish(leg, chunk):
        drain(x_leg.at[chunk, pl.ds(0, 3)], x_ssem.at[leg, chunk % 2], x_rsem.at[leg, chunk])
        drain(x_leg.at[chunk, 0], x_osem.at[leg, chunk % 2])

    def x_gather(chunk):
        def pick_plane(z, carry):
            x_send[chunk % 2, z] = pick_slots(plane_codes(chunk, 0, z), own_codes, x_rows)
            return carry

        lax.fori_loop(0, SIDE, pick_plane, 0)
        x_launch(0, chunk)

    def x_combine(chunk):
        x_finish(5, chunk)

        def add_plane(z, carry):
            y = x_back[chunk, z].reshape(SIDE * SIDE * BLK, d_model - rest)
            want = plane_codes(chunk, 0, z)
            for n in range(2):
                x_acc[n] += weigh_slots(want, own_codes, y, n)
            return carry

        lax.fori_loop(0, SIDE, add_plane, 0)

    x_acc[...] = jnp.zeros_like(x_acc)
    x_gather(0)
    for n in (node, other):
        for part in range(3):
            drain(rings[part].at[pl.ds(0, 2), n], a_send.at[part, n], a_recv.at[part, n])
            for c in ring_copies(part, n)[1]:
                c.start()
    for dim in range(3):
        drain(codes.at[dim, pl.ds(0, 3)], c_ssem.at[dim], c_rsem.at[dim])

    def line(ref, slot, part, k, index):
        idx = [slot, slice(None), slice(None), slice(None), slice(None), pl.ds(*cols[part])]
        idx[1 + ROUTES[part][0]], idx[1 + ROUTES[part][1]] = k, index
        return ref.at[tuple(idx)]

    def first_leg(chunk, part, k):
        dim = ROUTES[part][1]
        for v, shift in enumerate(SHIFTS):
            to_ep(line(send1, chunk % 2, part, k, (pos[dim] + shift) % SIDE), line(mid_d, chunk, part, k, pos[dim]),
                  send_sem.at[0, chunk % 2], recv_sem.at[0, chunk], dim, shift).start()
        pltpu.make_async_copy(line(send1, chunk % 2, part, k, pos[dim]), line(mid_d, chunk, part, k, pos[dim]),
                              own_sem.at[0, chunk % 2]).start()

    def last_leg(chunk, part, v):
        dim = ROUTES[part][1]
        k = (pos[ROUTES[part][0]] + v) % SIDE
        made = [to_ep(line(hop, chunk, part, k, (pos[dim] + shift) % SIDE), line(mid_r, chunk, part, k, pos[dim]),
                      l_send.at[v], l_recv.at[v], dim, shift) for shift in SHIFTS]
        return made + [pltpu.make_async_copy(line(hop, chunk, part, k, pos[dim]), line(mid_r, chunk, part, k, pos[dim]), l_own.at[v])]

    def last_finish(chunk, v):
        drain(mid_r.at[chunk, 0, pl.ds(0, 3), :, :, pl.ds(0, rest)], l_send.at[v], l_recv.at[v])
        drain(mid_r.at[chunk, 0, 0, :, :, pl.ds(0, rest)], l_own.at[v])

    def gather(chunk):
        for v in (0, 3, 1, 2):
            for part in range(3):
                if v == 2:
                    @pl.when(chunk == 0)
                    def _():
                        for n in (node, other):
                            drain(rings[part].at[0, n], b_send.at[part, n], b_recv.at[part, n])
                dim = ROUTES[part][0]
                k = (pos[dim] + v) % SIDE
                c0, width = cols[part]
                idx = [chunk % 2, slice(None), slice(None), slice(None), slice(None), slice(c0, c0 + width)]
                idx[1 + dim] = k
                send1[tuple(idx)] = pick_slots(plane_codes(chunk, dim, pos[dim]), codes.at[dim, k], rings[part].at[k])
                first_leg(chunk, part, k)

    def ffn(chunk):
        width = 256

        def up(n, carry):
            at = pl.ds(pl.multiple_of(n * width, width), width)
            x = work[chunk].reshape(rows, d_model)
            g = jnp.dot(x, wg[:, at], preferred_element_type=f32)
            u = jnp.dot(x, wu[:, at], preferred_element_type=f32)
            hid[:, at] = (jax.nn.silu(g) * u).astype(bf16)
            return carry

        lax.fori_loop(0, d_ff // width, up, 0)

        def down(n, carry):
            at = pl.ds(pl.multiple_of(n * width, width), width)
            y = jnp.dot(hid[...], wd[:, at], preferred_element_type=f32)
            work[chunk, :, :, :, :, at] = y.reshape(SIDE, SIDE, SIDE, BLK, width).astype(bf16)
            return carry

        lax.fori_loop(0, d_model // width, down, 0)

    def fold(chunk, v, part):
        dim = ROUTES[part][0]
        k = (pos[dim] + v) % SIDE
        c0, width = cols[part]
        want = plane_codes(chunk, dim, pos[dim])
        idx = [chunk, slice(None), slice(None), slice(None), slice(None), slice(c0, c0 + width)]
        idx[1 + dim] = k
        y = mid_r[tuple(idx)].reshape(SIDE * SIDE * BLK, width)
        for n in range(2):
            accs[part][k, n] += weigh_slots(want, codes.at[dim, k], y, n)

    def step(t, carry):
        @pl.when(t < n_chunks)
        def _():
            gather(t)
            x_finish(0, t)
            x_launch(1, t)

        @pl.when(t + 1 < n_chunks)
        def _():
            x_gather(t + 1)

        for stage in range(1, 5):
            chunk = t - stage

            @pl.when((chunk >= 0) & (chunk < (n_chunks if stage < 4 else n_chunks - 1)))
            def _():
                finish(stage - 1, chunk)
                x_finish(stage, chunk)
                if stage == 2:
                    @pl.when(chunk == 0)
                    def _():
                        for c in weights:
                            c.wait()
                    ffn(chunk)
                x_launch(stage + 1, chunk)
                if stage < 4:
                    launch(stage, chunk)
                else:
                    def fold_source(v, carry):
                        for part in range(3):
                            fold(chunk, v, part)
                        return carry

                    lax.fori_loop(0, SIDE, fold_source, 0)

        @pl.when(t >= 5)
        def _():
            x_combine(t - 5)

        return carry

    lax.fori_loop(0, n_chunks + 2, step, 0)

    def far_copies(part, n):
        dim = ROUTES[part][0]
        k = (pos[dim] + 2) % SIDE
        return [to_ep(accs[part].at[k, n, pl.ds(v * half, half)], fars[part].at[v, n], f_send.at[part, n], f_recv.at[part, n],
                      dim, (1, 3)[v]) for v in range(2)]

    first = (cols[0][1] // 128 + 1) // 2 * 128
    pieces = ((0, first), (first, cols[0][1] - first))

    def near_copies(part, n, piece):
        dim = ROUTES[part][0]
        span = pl.ds(*pieces[piece])
        return [to_ep(accs[part].at[(pos[dim] + (1, 3)[v]) % SIDE, n, :, span], nears[part].at[v, n, :, span],
                      n_send.at[part, n, piece], n_recv.at[part, n, piece], dim, (1, 3)[v]) for v in range(2)]

    last, prev = n_chunks - 1, n_chunks - 2

    finish(2, last)
    x_finish(3, last)

    def start_source(i, carry):
        for part in range(3):
            for c in last_leg(last, part, (2 + 3 * i) % SIDE):
                c.start()
        return carry

    lax.fori_loop(0, SIDE, start_source, 0)
    x_launch(4, last)
    finish(3, prev)
    x_finish(4, prev)
    x_launch(5, prev)

    def fold_far(i, carry):
        @pl.when(i == 1)
        def _():
            last_finish(last, 2)

        for part in range(3):
            fold(prev + i, 2, part)

            @pl.when(i == 1)
            def _():
                for c in far_copies(part, other):
                    c.start()
        return carry

    lax.fori_loop(0, 2, fold_far, 0)
    for part in range(3):
        for c in far_copies(part, node):
            c.start()
    x_combine(n_chunks - 3)
    x_finish(4, last)
    x_launch(5, last)

    def fold_rest(chunk, v):
        @pl.when(chunk == last)
        def _():
            last_finish(last, v)

        for part in range(3):
            fold(chunk, v, part)

    def fold_near(i, carry):
        fold_rest(prev + i // 2, 1 + 2 * (i % 2))
        return carry

    lax.fori_loop(0, 4, fold_near, 0)
    for n in (other, node):
        for part in range(3):
            i = pos[ROUTES[part][0]]
            drain(fars[part].at[:, n], f_send.at[part, n], f_recv.at[part, n])
            for v in range(2):
                accs[part][(i + (1, 3)[v]) % SIDE, n, v * half:(v + 1) * half] += fars[part][v, n]
        for piece in range(2):
            for part in range(3):
                for c in near_copies(part, n, piece):
                    c.start()

    def finish_own(i, carry):
        fold_rest(prev + i, 0)
        return carry

    lax.fori_loop(0, 2, finish_own, 0)

    def finish_x(i, carry):
        x_combine(prev + i)
        return carry

    lax.fori_loop(0, 2, finish_x, 0)

    def total(part, n, piece):
        drain(nears[part].at[:, n, :, pl.ds(*pieces[piece])], n_send.at[part, n, piece], n_recv.at[part, n, piece])
        at = slice(pieces[piece][0], pieces[piece][0] + pieces[piece][1])
        return (accs[part][pos[ROUTES[part][0]], n, :, at] + nears[part][0, n, :, at] + nears[part][1, n, :, at]).astype(bf16)

    def span_of(part, piece):
        return slice(cols[part][0] + pieces[piece][0], cols[part][0] + pieces[piece][0] + pieces[piece][1])

    def home(at, i):
        c = pltpu.make_async_copy(tok.at[:, pl.ds(at.start, at.stop - at.start)], out_ref.at[:, pl.ds(at.start, at.stop - at.start)], o_sem.at[0])
        c.start()
        return c

    for piece in range(2):
        for part in range(3):
            p_buf[other, :, span_of(part, piece)] = total(part, other, piece)
    p_buf[other, :, rest:] = x_acc[other].astype(bf16)
    share = to_pair(p_buf.at[other], p_recv, 4)
    share.start()
    x_sum = lax.dot_general(pick[node, :cap], x_acc[node].astype(bf16), TN, preferred_element_type=f32)
    share.wait()
    x_sum = x_sum + lax.dot_general(pick[other, :cap], p_recv[:, rest:], TN, preferred_element_type=f32)
    tok[:, rest:] = x_sum.astype(bf16)
    homes = [home(slice(rest, d_model), 0)]
    for part in range(3):
        at = slice(cols[part][0], cols[part][0] + cols[part][1])
        tok[:, at] = lax.dot_general(pick[other, :cap], p_recv[:, at], TN, preferred_element_type=f32).astype(bf16)
    for piece in range(2):
        for part in range(3):
            at = span_of(part, piece)
            mine = lax.dot_general(pick[node, :cap], total(part, node, piece), TN, preferred_element_type=f32)
            tok[:, at] = (tok[:, at].astype(f32) + mine).astype(bf16)
            homes.append(home(at, 1 + piece * 3 + part))
    drain(tok, o_sem.at[0])


def solution(mesh):
    n_nodes = mesh.shape['node']
    n_ep = mesh.shape['ep']
    row_spec = P(('dp', 'node', 'ep'), None)
    exp_spec = P(('node', 'ep'), None, None)

    def local_layer(tokens, expert_ids, route_w, node_slot, exp_slot, w_gate, w_up, w_down):
        tok_dev, d_model = tokens.shape
        top_k = expert_ids.shape[1]
        d_ff = w_gate.shape[2]
        n_exp = w_gate.shape[0] * n_ep * n_nodes
        limit = max(1, min(top_k, n_nodes // 2))
        cap_node = min(tok_dev, 8 * ((5 * tok_dev * limit + 32 * n_nodes - 1) // (32 * n_nodes)))
        cap_exp = 8 * ((5 * n_nodes * tok_dev * top_k + 32 * n_exp - 1) // (32 * n_exp))
        n_chunks = cap_exp // BLK
        rows = n_ep * BLK

        cube = (SIDE, SIDE, SIDE, BLK, d_model)
        wide = d_model - 3 * part_columns(d_model)[0][1]
        x_cube = (SIDE, SIDE, SIDE, BLK, wide)
        bf16, f32, i32 = jnp.bfloat16, jnp.float32, jnp.int32
        any_spec = pl.BlockSpec(memory_space=pl.ANY)
        dma = pltpu.SemaphoreType.DMA
        out, _, _ = pl.pallas_call(
            functools.partial(moe_kernel, n_chunks),
            name="moe_layer",
            out_shape=(jax.ShapeDtypeStruct((tok_dev, d_model), bf16),
                       jax.ShapeDtypeStruct((n_chunks,) + cube, bf16),
                       jax.ShapeDtypeStruct((n_chunks,) + cube, bf16)),
            in_specs=[any_spec] * 8,
            out_specs=(any_spec, any_spec, any_spec),
            scratch_shapes=[
                pltpu.VMEM((top_k, tok_dev), i32), pltpu.VMEM((top_k, tok_dev), f32),
                pltpu.VMEM((top_k, tok_dev), i32), pltpu.VMEM((top_k, tok_dev), i32),
                pltpu.VMEM((tok_dev, d_model), bf16),
                pltpu.VMEM((2, tok_dev, tok_dev), bf16),
                *[pltpu.VMEM((SIDE, 2, cap_node, width), bf16) for _, width in part_columns(d_model)],
                pltpu.VMEM((2, 2 * top_k, tok_dev), f32), pltpu.VMEM((3, SIDE, 2, 2 * top_k, tok_dev), f32), pltpu.VMEM((2 * top_k, tok_dev), f32),
                pltpu.VMEM((2, cap_node, d_model), bf16), pltpu.VMEM((cap_node, d_model), bf16),
                pltpu.VMEM((2, cap_node, wide), bf16), pltpu.VMEM((2,) + x_cube, bf16), pltpu.VMEM((n_chunks,) + x_cube, bf16),
                pltpu.VMEM((n_chunks,) + x_cube, bf16), pltpu.VMEM((2, cap_node, wide), f32),
                pltpu.VMEM((d_model, d_ff), bf16), pltpu.VMEM((d_model, d_ff), bf16), pltpu.VMEM((d_ff, d_model), bf16),
                pltpu.VMEM((2,) + cube, bf16), pltpu.VMEM((n_chunks,) + cube, bf16), pltpu.VMEM((n_chunks,) + cube, bf16),
                pltpu.VMEM((rows, d_ff), bf16),
                *[pltpu.VMEM((SIDE, 2, cap_node, width), f32) for _, width in part_columns(d_model)],
                *[pltpu.VMEM((2, 2, cap_node // 2, width), f32) for _, width in part_columns(d_model)],
                *[pltpu.VMEM((2, 2, cap_node, width), f32) for _, width in part_columns(d_model)],
                dma((5,)), dma((3,)), dma((4, 2)), dma((4, 2)), dma((4, n_chunks)), dma((9,)), dma((9,)),
                dma((3, 2)), dma((3, 2)), dma((3, 2)), dma((3, 2)), dma((3,)), dma((3,)),
                dma((3, 2)), dma((3, 2)), dma((3, 2, 2)), dma((3, 2, 2)),
                dma((6, 2)), dma((6, n_chunks)), dma((6, 2)),
                dma((4,)), dma((4,)), dma((4,)), dma((1,)),
            ],
            compiler_params=pltpu.CompilerParams(collective_id=0, has_side_effects=True, vmem_limit_bytes=67_043_328),
        )(expert_ids.T, route_w.T, node_slot.T, exp_slot.T, tokens, w_gate[0], w_up[0], w_down[0])
        return out

    return jax.shard_map(local_layer, mesh=mesh, in_specs=(row_spec,) * 5 + (exp_spec,) * 3, out_specs=row_spec, check_vma=False)
```
